512 devices in a mesh: dp: 8 (over y), slab: 16 (over x_hi, z), view: 4 (over x_lo, core).
Axes of the slice: x: 4 (x_hi: 2, x_lo: 2; x = x_hi * 2 + x_lo), y: 8, z: 8, core: 2. Of those that a mesh axis runs over, the one named last changes fastest.
Arguments:
- latent_feats: bfloat16 [8, 4, 64, 32, 256], P('dp', 'view', 'slab'), may hold values from -6 to 6
- conv_weight: bfloat16 [2304, 256], P(('dp', 'slab')), may hold values from -0.125 to 0.125
- kv_weight: bfloat16 [256, 1536], P(('dp', 'slab')), may hold values from -0.375 to 0.375
- stream: bfloat16 [8, 4, 64, 32, 768], P('dp', 'view', 'slab'), may hold values from -6 to 6
- queries: bfloat16 [8, 4, 64, 32, 768], P('dp', 'view', 'slab'), may hold values from -102 to 102
- norm_gain: float32 [768], replicated, may hold values from 0.1 to 1.9
- up_weight: bfloat16 [768, 3072], P(('dp', 'slab'), 'view'), may hold values from -0.21875 to 0.21875
- down_weight: bfloat16 [768, 3072], P(('dp', 'slab'), 'view'), may hold values from -0.109375 to 0.109375
- band_start: int32 [8, 4, 64, 4], P('dp', 'view', 'slab'), may hold values from 0 to 63, as said below
- band_end: int32 [8, 4, 64, 4], P('dp', 'view', 'slab'), may hold values from 1 to 64
- visibility: int32 [8, 4, 4], P('dp'), may hold values 0 or 1
Outputs:
- output: bfloat16 [8, 4, 64, 32, 768], P('dp', 'view', 'slab')
The draws below stay inside these ranges and needn't reach their ends.
Inputs may be any that keep to these rules, and one draw needn't show every extreme that they name: band_end - band_start lies in 1 to 4 and equals 4 for some rows in every draw; for a row r both bounds lie within rows (r // 4) * 4 - 1 to (r // 4 + 1) * 4 + 1, clipped to the grid.
All inputs are finite; a program needn't handle non-finite values. No bound on the sum of `visibility` on one device may be relied on, other than what follows from the above.
Results may differ from the reference program's by a relative error of at most 0.0085.
Values may be sent and summed in bfloat16 or wider, within the bound.
No kernel may reach another device: no remote copies, remote signals or barrier semaphores. Data moves between devices by JAX's collectives and lax.ppermute only.
A program may use at most 64 MiB of HBM per device.

```python
import jax
import jax.numpy as jnp
from jax import lax

D = 768
HEADS = 12
HEAD_DIM = 64
FF = 3072
C = 256
ROWS_DEV = 4
HALO = 1
BAND = 4
COLS = 32
SCENES = 8
VIEWS = 4
HEIGHT = 64
UNIT_GROUPS = 4
FF_GROUP = 768
N_SLAB = 16


def band_pair(key):
    base_key = jax.random.fold_in(key, 7)
    key_length, key_offset = jax.random.split(base_key)
    full_shape = (SCENES, VIEWS, HEIGHT, VIEWS)
    row_ids = jnp.arange(HEIGHT, dtype=jnp.int32).reshape(1, 1, HEIGHT, 1)
    block_top = row_ids // ROWS_DEV * ROWS_DEV
    lowest = jnp.maximum(block_top - HALO, 0)
    highest = jnp.minimum(block_top + ROWS_DEV + HALO, HEIGHT)
    length = jax.random.randint(key_length, full_shape, 1, BAND + 1)
    view_ids = jnp.arange(VIEWS, dtype=jnp.int32).reshape(1, VIEWS, 1, 1)
    other_ids = jnp.arange(VIEWS, dtype=jnp.int32).reshape(1, 1, 1, VIEWS)
    forced = row_ids == (view_ids + 5 * other_ids) % HEIGHT
    length = jnp.where(forced, BAND, length)
    room_left = jnp.broadcast_to(highest - lowest - length + 1, full_shape)
    offset = jax.random.randint(key_offset, full_shape, 0, room_left)
    first_rows = jnp.broadcast_to(lowest, full_shape) + offset
    return (first_rows.astype(jnp.int32), (first_rows + length).astype(jnp.int32))


def draw_band_start(key, part):
    return band_pair(key)[0]


def draw_band_end(key, part):
    return band_pair(key)[1]


def draw_queries(key, part):
    full_shape = (SCENES, VIEWS, HEIGHT, COLS, D)
    key_base = jax.random.fold_in(jax.random.fold_in(key, 11), 0)
    values = jnp.clip(jax.random.normal(key_base, full_shape, jnp.float32), -6.0, 6.0)
    return values.astype(jnp.bfloat16)


def place_ends(values, own_key, least, top_value):
    spot = [jax.random.randint(jax.random.fold_in(own_key, axis), (), 0, length) for axis, length in enumerate(values.shape)]
    longest = values.shape.index(max(values.shape))
    neighbour = spot[:longest] + [(spot[longest] + 1) % values.shape[longest]] + spot[longest + 1:]
    return values.at[tuple(spot)].set(least).at[tuple(neighbour)].set(top_value)


def block_scale(own_key, shape, pieces, least, high):
    loudness = 1.0
    for axis_at, shards_of in pieces:
        steps = jax.random.uniform(jax.random.fold_in(jax.random.fold_in(own_key, 6), axis_at), (shards_of,), jnp.float32, least / len(pieces), high / len(pieces))
        loudness = loudness * jnp.repeat(jnp.exp(steps), shape[axis_at] // shards_of).reshape((-1,) + (1,) * (len(shape) - 1 - axis_at))
    return loudness


def bell_draw(own_key, dims, scale, most, cuts=(), held_as=jnp.bfloat16):
    array = scale * jax.random.normal(own_key, dims, jnp.float32)
    if cuts:
        array = array * block_scale(own_key, dims, cuts, -0.22, 0.18)
    return jnp.clip(array, -most, most).astype(held_as)


def setup_inputs(seed: int = 0) -> dict:
    seeds = jax.random.split(jax.random.key(seed), 12)
    latent_feats = bell_draw(seeds[0], (SCENES, VIEWS, HEIGHT, COLS, C), 1.0, 6.0, ((0, 8), (1, 4), (2, 16)))
    conv_weight = bell_draw(seeds[1], (9 * C, C), (9 * C) ** -0.5, 0.125, ((0, 128),))
    kv_weight = bell_draw(seeds[2], (C, 2 * D), C ** -0.5, 0.375, ((0, 128),))
    stream = bell_draw(seeds[3], (SCENES, VIEWS, HEIGHT, COLS, D), 1.0, 6.0, ((0, 8), (1, 4), (2, 16)))
    queries = draw_queries(jax.random.fold_in(seeds[11], 71), 0)
    norm_gain = jnp.clip(1.0 + 0.18 * jax.random.normal(seeds[5], (D,), jnp.float32), 0.1, 1.9)
    up_weight = bell_draw(seeds[6], (D, FF), D ** -0.5, 0.21875, ((0, 128), (1, 4)))
    down_weight = bell_draw(seeds[7], (D, FF), FF ** -0.5, 0.109375, ((0, 128), (1, 4)))
    band_start = draw_band_start(jax.random.fold_in(seeds[11], 71), 0)
    band_end = draw_band_end(jax.random.fold_in(seeds[11], 71), 0)
    visibility = place_ends((jax.random.randint(seeds[10], (SCENES, VIEWS, VIEWS), 0, 2) < 1).astype(jnp.int32), jax.random.fold_in(seeds[10], 1), 0, 1)
    return {"latent_feats": latent_feats, "conv_weight": conv_weight, "kv_weight": kv_weight, "stream": stream, "queries": queries, "norm_gain": norm_gain, "up_weight": up_weight, "down_weight": down_weight, "band_start": band_start, "band_end": band_end, "visibility": visibility}


def conv_layer(view_feats, conv_weight):
    height, col_count, channels = view_feats.shape
    padded = jnp.pad(view_feats, ((1, 1), (1, 1), (0, 0)))
    running = jnp.zeros((height * col_count, channels), jnp.float32)
    for tap_index in range(9):
        row_off = tap_index // 3
        col_off = tap_index % 3
        window = padded[row_off:row_off + height, col_off:col_off + col_count].reshape(-1, channels)
        taps = conv_weight[tap_index * channels:(tap_index + 1) * channels]
        running = running + jnp.dot(window, taps, preferred_element_type=jnp.float32)
    summed = view_feats.reshape(-1, channels).astype(jnp.float32) + jax.nn.silu(running)
    return summed.astype(jnp.bfloat16).reshape(height, col_count, channels)

def band_attention(query_rows, near_kv, block_starts, block_ends, vis_row, view_id, first_row):
    near_rows = near_kv.shape[1]
    keys = near_kv[..., :D].reshape(-1, HEADS, HEAD_DIM).astype(jnp.float32)
    values = near_kv[..., D:].reshape(-1, HEADS, HEAD_DIM).astype(jnp.float32)
    key_rows = first_row - HALO + jnp.arange(near_rows, dtype=jnp.int32)
    inside = (block_starts[:, :, None] <= key_rows) & (key_rows < block_ends[:, :, None])
    seen = (jnp.arange(VIEWS, dtype=jnp.int32) == view_id) | (vis_row == 1)
    allowed = inside & seen[None, :, None]
    allowed = jnp.broadcast_to(allowed[:, None, :, :, None], (ROWS_DEV, COLS, VIEWS, near_rows, COLS))
    allowed = allowed.reshape(ROWS_DEV * COLS, -1)
    query_heads = query_rows.reshape(-1, HEADS, HEAD_DIM).astype(jnp.float32)
    scores = jnp.einsum('qhd,khd->hqk', query_heads, keys) * HEAD_DIM ** (-0.5)
    scores = jnp.where(allowed[None], scores, -1e+30)
    highest = lax.optimization_barrier(jnp.max(scores, axis=-1, keepdims=True))
    weights = jnp.exp(scores - highest)
    weights = weights / lax.optimization_barrier(jnp.sum(weights, axis=-1, keepdims=True))
    probs = lax.optimization_barrier(weights.astype(jnp.bfloat16)).astype(jnp.float32)
    return jnp.einsum('hqk,khd->qhd', probs, values).reshape(-1, D)

def reference(latent_feats, conv_weight, kv_weight, stream, queries, norm_gain, up_weight, down_weight, band_start, band_end, visibility):

    def scene_pass(operands):
        scene_feats, scene_stream, scene_queries, scene_starts, scene_ends, scene_visible = operands
        encoded = jnp.stack([conv_layer(scene_feats[view_index], conv_weight) for view_index in range(VIEWS)])
        projected = jnp.dot(encoded.reshape(-1, C), kv_weight, preferred_element_type=jnp.float32)
        projected = projected.astype(jnp.bfloat16).reshape(VIEWS, HEIGHT, COLS, 2 * D)
        padded = jnp.pad(projected, ((0, 0), (HALO, HALO), (0, 0), (0, 0)))

        def block_pass(block_index):
            view_id = (block_index // N_SLAB).astype(jnp.int32)
            first_row = (block_index % N_SLAB * ROWS_DEV).astype(jnp.int32)
            near_kv = lax.dynamic_slice_in_dim(padded, first_row, ROWS_DEV + 2 * HALO, 1)
            view_queries = lax.dynamic_index_in_dim(scene_queries, view_id, 0, False)
            query_rows = lax.dynamic_slice_in_dim(view_queries, first_row, ROWS_DEV, 0).reshape(-1, D)
            view_starts = lax.dynamic_index_in_dim(scene_starts, view_id, 0, False)
            view_ends = lax.dynamic_index_in_dim(scene_ends, view_id, 0, False)
            block_starts = lax.dynamic_slice_in_dim(view_starts, first_row, ROWS_DEV, 0)
            block_ends = lax.dynamic_slice_in_dim(view_ends, first_row, ROWS_DEV, 0)
            vis_row = lax.dynamic_index_in_dim(scene_visible, view_id, 0, False)
            return band_attention(query_rows, near_kv, block_starts, block_ends, vis_row, view_id, first_row)
        attended = lax.map(block_pass, jnp.arange(VIEWS * N_SLAB, dtype=jnp.int32))
        attended = attended.reshape(VIEWS * HEIGHT * COLS, D)
        residual = scene_stream.reshape(-1, D).astype(jnp.float32) + attended
        square_mean = lax.optimization_barrier(jnp.mean(residual * residual, axis=-1, keepdims=True))
        normed = (residual * lax.rsqrt(square_mean + 1e-06) * norm_gain).astype(jnp.bfloat16)
        hidden = jax.nn.gelu(jnp.dot(normed, up_weight, preferred_element_type=jnp.float32), approximate=True)
        hidden = hidden.astype(jnp.bfloat16)
        mixed = jnp.zeros((VIEWS * HEIGHT * COLS, D), jnp.float32)
        for group_index in range(UNIT_GROUPS):
            lower = group_index * FF_GROUP
            term = lax.dot_general(hidden[:, lower:lower + FF_GROUP], down_weight[:, lower:lower + FF_GROUP], (((1,), (1,)), ((), ())), preferred_element_type=jnp.float32)
            term = lax.optimization_barrier(term.astype(jnp.bfloat16))
            mixed = mixed + term.astype(jnp.float32)
        return (residual + mixed).astype(jnp.bfloat16).reshape(VIEWS, HEIGHT, COLS, D)
    return lax.map(scene_pass, (latent_feats, stream, queries, band_start, band_end, visibility))
```

```python
import functools

import jax
import jax.numpy as jnp
from jax import lax
from jax.experimental import pallas as pl
from jax.experimental.pallas import tpu as pltpu
from jax.sharding import Mesh
from jax.sharding import PartitionSpec as P

HEADS = 12
HEAD_DIM = 64
SLAB = ("slab_0", "slab_1")
DP_SLAB = ("dp", "slab_0", "slab_1")
BF = jnp.bfloat16
F32 = jnp.float32

VMEM = pl.BlockSpec(memory_space=pltpu.VMEM)
SMEM = pl.BlockSpec(memory_space=pltpu.SMEM)


def conv_kernel(where_ref, x_ref, own_ref, other_ref, out_ref):
    first = where_ref[0] == 0
    x = x_ref[...].astype(F32)
    col = lax.broadcasted_iota(jnp.int32, x.shape, 0) % 32
    left = jnp.where(col == 0, 0.0, pltpu.roll(x, 1, 0)).astype(BF)
    right = jnp.where(col == 31, 0.0, pltpu.roll(x, x.shape[0] - 1, 0)).astype(BF)
    shifted = (left, x_ref[...], right)
    halves = []
    for ref in (own_ref, other_ref):
        halves.append(jnp.concatenate([ref[d, 0:288, :] for d in range(8)], axis=0))
    weight = jnp.concatenate(halves, axis=1)
    acc = jnp.zeros((192, 256), F32)
    for tap in range(9):
        rows = shifted[tap % 3][tap // 3 * 32 : tap // 3 * 32 + 192]
        acc = acc + jnp.dot(
            rows, weight[tap * 256 : (tap + 1) * 256], preferred_element_type=F32
        )
    low = jnp.where(first, acc[:, :128], acc[:, 128:])
    high = jnp.where(first, acc[:, 128:], acc[:, :128])
    conv = jnp.concatenate([low, high], axis=1)
    silu = conv / (1.0 + jnp.exp(-conv))
    out_ref[...] = (x[32:224] + silu).astype(BF)


def attention_kernel(
    where_ref,
    start_ref,
    end_ref,
    seen_ref,
    enc_ref,
    own_ref,
    other_ref,
    q_ref,
    stream_ref,
    gain_ref,
    normed_ref,
    residual_ref,
    kv_ref,
    bias_ref,
):
    first = where_ref[0] == 0
    first_row = where_ref[1]
    enc = enc_ref[...]
    for half in range(2):
        for tile in range(6):
            own = jnp.concatenate(
                [own_ref[d, 288 + tile * 32 : 320 + tile * 32, :] for d in range(8)], axis=0
            )
            other = jnp.concatenate(
                [other_ref[d, 288 + tile * 32 : 320 + tile * 32, :] for d in range(8)], axis=0
            )
            weight = jnp.where(first, own, other) if half == 0 else jnp.where(first, other, own)
            kv = jnp.dot(enc, weight, preferred_element_type=F32)
            kv_ref[half * 6 + tile] = kv.astype(BF)
    lane = lax.broadcasted_iota(jnp.int32, (1, 768), 1)
    key_view = lane // 192
    key_row = first_row - 1 + (lane % 192) // 32
    for r in range(4):
        low = jnp.zeros((1, 768), jnp.int32)
        high = jnp.zeros((1, 768), jnp.int32)
        for u in range(4):
            mine = key_view == u
            low = jnp.where(mine, start_ref[r, u], low)
            high = jnp.where(mine, jnp.where(seen_ref[u] == 1, end_ref[r, u], -1), high)
        bias = jnp.where((low <= key_row) & (key_row < high), 0.0, -1e30)
        bias_ref[r * 32 : (r + 1) * 32, :] = jnp.broadcast_to(bias, (32, 768))
    left = lax.broadcasted_iota(jnp.int32, (128, 128), 1) < HEAD_DIM
    square = jnp.zeros((128, 1), F32)
    for pair in range(6):
        half, tile = pair // 3, pair % 3
        q = q_ref[:, pair * 128 : (pair + 1) * 128]
        zero = jnp.zeros_like(q)
        keys = kv_ref[half * 6 + tile]
        values = kv_ref[half * 6 + 3 + tile]
        outs = []
        for side in range(2):
            mine = left if side == 0 else ~left
            scores = lax.dot_general(
                jnp.where(mine, q, zero), keys, (((1,), (1,)), ((), ())), preferred_element_type=F32
            )
            scores = scores * HEAD_DIM ** (-0.5) + bias_ref[...]
            weights = jnp.exp(scores - jnp.max(scores, axis=-1, keepdims=True))
            total = jnp.sum(weights, axis=-1, keepdims=True)
            probs = (weights / total).astype(BF)
            outs.append(jnp.dot(probs, values, preferred_element_type=F32))
        attended = jnp.where(left, outs[0], outs[1])
        cols = slice(pair * 128, (pair + 1) * 128)
        residual = stream_ref[:, cols].astype(F32) + attended
        residual_ref[:, cols] = residual
        square = square + jnp.sum(residual * residual, axis=-1, keepdims=True)
    scale = lax.rsqrt(square * (1.0 / 768) + 1e-6)
    normed_ref[...] = (residual_ref[...] * scale * gain_ref[...]).astype(BF)


def gelu(v):
    return 0.5 * v * (1.0 + jnp.tanh(0.7978845608028654 * (v + 0.044715 * (v * v * v))))


def mlp_kernel(tok_ref, w_ref, out_ref, up_ref, down_ref):
    for tile in range(6):
        for d in range(8):
            up_ref[d * 96 : (d + 1) * 96, tile * 128 : (tile + 1) * 128] = w_ref[
                d, tile * 96 : (tile + 1) * 96, :
            ]
            down_ref[d * 96 : (d + 1) * 96, tile * 128 : (tile + 1) * 128] = w_ref[
                d, 576 + tile * 96 : 576 + (tile + 1) * 96, :
            ]
    for block in range(4):
        rows = slice(block * 128, (block + 1) * 128)
        hidden = gelu(jnp.dot(tok_ref[rows, :], up_ref[...], preferred_element_type=F32))
        out_ref[block] = lax.dot_general(
            hidden.astype(BF), down_ref[...], (((1,), (1,)), ((), ())), preferred_element_type=F32
        ).astype(BF)


def kernel_call(body, out_shape, in_specs, scratch=(), name=None):
    outs = jax.tree.map(lambda _: VMEM, out_shape)
    return pl.pallas_call(
        body,
        out_shape=out_shape,
        in_specs=in_specs,
        out_specs=outs,
        scratch_shapes=scratch,
        name=name,
        compiler_params=pltpu.CompilerParams(vmem_limit_bytes=32 << 20),
    )


def copy_for_each(value, axes):
    count = 1
    for axis in axes:
        count *= lax.axis_size(axis)
    copies = jnp.broadcast_to(value, (count, *value.shape))
    return lax.all_to_all(copies, axes, split_axis=0, concat_axis=0, tiled=True)


def tile_columns(weight):
    rows, cols = weight.shape
    return weight.reshape(rows, cols // 128, 128).swapaxes(0, 1).reshape(-1, 128)


def regroup(tiles, rows):
    devices = tiles.shape[0]
    tiles = tiles.reshape(devices, -1, rows, 128).swapaxes(0, 1)
    return tiles.reshape(-1, 128)


def shards(
    latent_feats,
    conv_weight,
    kv_weight,
    stream,
    queries,
    norm_gain,
    up_weight,
    down_weight,
    band_start,
    band_end,
    visibility,
):
    view_id = lax.axis_index("view")
    core = view_id % 2
    first_row = lax.axis_index(SLAB) * 4
    where = jnp.stack([core, first_row]).astype(jnp.int32)
    feats = latent_feats[0, 0]
    ends = lax.axis_size(SLAB) - 1
    above = lax.ppermute(feats[2:], SLAB, [(i, i + 1) for i in range(ends)])
    below = lax.ppermute(feats[:2], SLAB, [(i + 1, i) for i in range(ends)])
    rows = jnp.concatenate([above, feats, below], axis=0).reshape(256, 256)

    conv_half = jnp.where(core == 0, conv_weight[:, :128], conv_weight[:, 128:])
    kv_half = jnp.where(
        core == 0,
        jnp.concatenate([kv_weight[:, :384], kv_weight[:, 768:1152]], axis=1),
        jnp.concatenate([kv_weight[:, 384:768], kv_weight[:, 1152:]], axis=1),
    )
    mine = jnp.concatenate(
        [conv_half, tile_columns(kv_half), tile_columns(up_weight), tile_columns(down_weight)],
        axis=0,
    )
    slabs = copy_for_each(mine, SLAB)
    code = jnp.concatenate([regroup(slabs[:, :18], 18), regroup(slabs[:, 18:30], 2)], axis=0)
    units = jnp.concatenate([regroup(slabs[:, 30:66], 6), regroup(slabs[:, 66:], 6)], axis=0)
    own = copy_for_each(code, ("dp",))
    other = lax.ppermute(own, "view", [(i, i ^ 1) for i in range(4)])
    mlp = copy_for_each(units, ("dp",))

    encoded = kernel_call(
        conv_kernel,
        jax.ShapeDtypeStruct((192, 256), BF),
        [SMEM, VMEM, VMEM, VMEM],
        name="encode",
    )(where, rows, own, other)
    nearby = lax.all_gather(encoded, "view", axis=0, tiled=True)
    vis_row = lax.dynamic_index_in_dim(visibility[0], view_id, 0, False)
    seen = jnp.where(jnp.arange(4) == view_id, 1, vis_row).astype(jnp.int32)
    normed, residual = kernel_call(
        attention_kernel,
        (jax.ShapeDtypeStruct((128, 768), BF), jax.ShapeDtypeStruct((128, 768), F32)),
        [SMEM, SMEM, SMEM, SMEM] + [VMEM] * 6,
        scratch=[pltpu.VMEM((12, 768, 128), BF), pltpu.VMEM((128, 768), F32)],
        name="attend",
    )(
        where,
        band_start[0, 0],
        band_end[0, 0],
        seen,
        nearby,
        own,
        other,
        queries[0, 0].reshape(128, 768),
        stream[0, 0].reshape(128, 768),
        norm_gain.reshape(1, 768),
    )
    tokens = lax.all_gather(normed, "view", axis=0, tiled=True)
    parts = kernel_call(
        mlp_kernel,
        jax.ShapeDtypeStruct((4, 128, 768), BF),
        [VMEM, VMEM],
        scratch=[pltpu.VMEM((768, 768), BF), pltpu.VMEM((768, 768), BF)],
        name="mlp",
    )(tokens, mlp)
    arrived = lax.all_to_all(parts, "view", split_axis=0, concat_axis=0, tiled=True)
    mixed = arrived.astype(F32).sum(axis=0)
    return (residual + mixed).astype(BF).reshape(1, 1, 4, 32, 768)


def solution(mesh):
    finer = Mesh(
        mesh.devices.reshape(mesh.shape["dp"], 2, 8, mesh.shape["view"]),
        ("dp", "slab_0", "slab_1", "view"),
    )
    in_specs = (
        P("dp", "view", SLAB, None, None),
        P(DP_SLAB, None),
        P(DP_SLAB, None),
        P("dp", "view", SLAB, None, None),
        P("dp", "view", SLAB, None, None),
        P(),
        P(DP_SLAB, "view"),
        P(DP_SLAB, "view"),
        P("dp", "view", SLAB, None),
        P("dp", "view", SLAB, None),
        P("dp", None, None),
    )
    out_specs = P("dp", "view", SLAB, None, None)
    return jax.shard_map(
        shards, mesh=finer, in_specs=in_specs, out_specs=out_specs, check_vma=False
    )
```

```python
import functools

import jax
import jax.numpy as jnp
from jax import lax
from jax.experimental import pallas as pl
from jax.experimental.pallas import tpu as pltpu
from jax.sharding import Mesh
from jax.sharding import PartitionSpec as P

HEADS = 12
HEAD_DIM = 64
SLAB = ("slab_0", "slab_1")
DP_SLAB = ("dp", "slab_0", "slab_1")
BF = jnp.bfloat16
F32 = jnp.float32

VMEM = pl.BlockSpec(memory_space=pltpu.VMEM)
SMEM = pl.BlockSpec(memory_space=pltpu.SMEM)


def slot(where_ref, d):
    return (where_ref[2] + 8 - d) % 8


def conv_kernel(where_ref, x_ref, own_ref, other_ref, out_ref):
    first = where_ref[0] == 0
    x = x_ref[...].astype(F32)
    col = lax.broadcasted_iota(jnp.int32, x.shape, 0) % 32
    left = jnp.where(col == 0, 0.0, pltpu.roll(x, 1, 0)).astype(BF)
    right = jnp.where(col == 31, 0.0, pltpu.roll(x, x.shape[0] - 1, 0)).astype(BF)
    shifted = (left, x_ref[...], right)
    halves = []
    for ref in (own_ref, other_ref):
        halves.append(
            jnp.concatenate([ref[slot(where_ref, d), 0:288, :] for d in range(8)], axis=0)
        )
    weight = jnp.concatenate(halves, axis=1)
    acc = jnp.zeros((192, 256), F32)
    for tap in range(9):
        rows = shifted[tap % 3][tap // 3 * 32 : tap // 3 * 32 + 192]
        acc = acc + jnp.dot(
            rows, weight[tap * 256 : (tap + 1) * 256], preferred_element_type=F32
        )
    low = jnp.where(first, acc[:, :128], acc[:, 128:])
    high = jnp.where(first, acc[:, 128:], acc[:, :128])
    conv = jnp.concatenate([low, high], axis=1)
    silu = conv / (1.0 + jnp.exp(-conv))
    out_ref[...] = (x[32:224] + silu).astype(BF)


def attention_kernel(
    where_ref,
    start_ref,
    end_ref,
    seen_ref,
    enc_ref,
    own_ref,
    other_ref,
    q_ref,
    stream_ref,
    gain_ref,
    normed_ref,
    residual_ref,
    kv_ref,
    bias_ref,
):
    first = where_ref[0] == 0
    first_row = where_ref[1]
    enc = enc_ref[...]
    for half in range(2):
        for tile in range(6):
            own = jnp.concatenate(
                [
                    own_ref[slot(where_ref, d), 288 + tile * 32 : 320 + tile * 32, :]
                    for d in range(8)
                ],
                axis=0,
            )
            other = jnp.concatenate(
                [
                    other_ref[slot(where_ref, d), 288 + tile * 32 : 320 + tile * 32, :]
                    for d in range(8)
                ],
                axis=0,
            )
            weight = jnp.where(first, own, other) if half == 0 else jnp.where(first, other, own)
            kv = jnp.dot(enc, weight, preferred_element_type=F32)
            kv_ref[half * 6 + tile] = kv.astype(BF)
    lane = lax.broadcasted_iota(jnp.int32, (1, 768), 1)
    key_view = lane // 192
    key_row = first_row - 1 + (lane % 192) // 32
    for r in range(4):
        low = jnp.zeros((1, 768), jnp.int32)
        high = jnp.zeros((1, 768), jnp.int32)
        for u in range(4):
            mine = key_view == u
            low = jnp.where(mine, start_ref[r, u], low)
            high = jnp.where(mine, jnp.where(seen_ref[u] == 1, end_ref[r, u], -1), high)
        bias = jnp.where((low <= key_row) & (key_row < high), 0.0, -1e30)
        bias_ref[r * 32 : (r + 1) * 32, :] = jnp.broadcast_to(bias, (32, 768))
    left = lax.broadcasted_iota(jnp.int32, (128, 128), 1) < HEAD_DIM
    square = jnp.zeros((128, 1), F32)
    for pair in range(6):
        half, tile = pair // 3, pair % 3
        q = q_ref[:, pair * 128 : (pair + 1) * 128]
        zero = jnp.zeros_like(q)
        keys = kv_ref[half * 6 + tile]
        values = kv_ref[half * 6 + 3 + tile]
        outs = []
        for side in range(2):
            mine = left if side == 0 else ~left
            scores = lax.dot_general(
                jnp.where(mine, q, zero), keys, (((1,), (1,)), ((), ())), preferred_element_type=F32
            )
            scores = scores * HEAD_DIM ** (-0.5) + bias_ref[...]
            weights = jnp.exp(scores - jnp.max(scores, axis=-1, keepdims=True))
            total = jnp.sum(weights, axis=-1, keepdims=True)
            probs = (weights / total).astype(BF)
            outs.append(jnp.dot(probs, values, preferred_element_type=F32))
        attended = jnp.where(left, outs[0], outs[1])
        cols = slice(pair * 128, (pair + 1) * 128)
        residual = stream_ref[:, cols].astype(F32) + attended
        residual_ref[:, cols] = residual
        square = square + jnp.sum(residual * residual, axis=-1, keepdims=True)
    scale = lax.rsqrt(square * (1.0 / 768) + 1e-6)
    normed_ref[...] = (residual_ref[...] * scale * gain_ref[...]).astype(BF)


def gelu(v):
    return 0.5 * v * (1.0 + jnp.tanh(0.7978845608028654 * (v + 0.044715 * (v * v * v))))


def mlp_kernel(where_ref, tok_ref, *refs):
    (*full_refs, up4_ref, down4_ref, out_ref, up_ref, down_ref) = refs
    here = where_ref[2]
    sources = [(k, ref, 0, ref, 576) for k, ref in zip((0, 1, 2, 3, 7, 6, 5), full_refs)]
    sources.append((4, up4_ref, 0, down4_ref, 0))
    for back, up_src, up_at, down_src, down_at in sources:
        row = pl.multiple_of((here + 8 - back) % 8 * 96, 16)
        for tile in range(6):
            cols = slice(tile * 128, (tile + 1) * 128)
            at = tile * 96
            up_ref[pl.ds(row, 96), cols] = up_src[up_at + at : up_at + at + 96, :]
            down_ref[pl.ds(row, 96), cols] = down_src[down_at + at : down_at + at + 96, :]
    for block in range(4):
        rows = slice(block * 128, (block + 1) * 128)
        hidden = gelu(jnp.dot(tok_ref[rows, :], up_ref[...], preferred_element_type=F32))
        out_ref[block] = lax.dot_general(
            hidden.astype(BF), down_ref[...], (((1,), (1,)), ((), ())), preferred_element_type=F32
        ).astype(BF)


def kernel_call(body, out_shape, in_specs, scratch=(), name=None):
    outs = jax.tree.map(lambda _: VMEM, out_shape)
    return pl.pallas_call(
        body,
        out_shape=out_shape,
        in_specs=in_specs,
        out_specs=outs,
        scratch_shapes=scratch,
        name=name,
        compiler_params=pltpu.CompilerParams(vmem_limit_bytes=16 << 20),
    )


def copy_for_each(value, axes):
    count = 1
    for axis in axes:
        count *= lax.axis_size(axis)
    copies = jnp.broadcast_to(value, (count, *value.shape))
    return lax.all_to_all(copies, axes, split_axis=0, concat_axis=0, tiled=True)


def hop(value, step):
    count = lax.axis_size("dp")
    return lax.ppermute(value, "dp", [(i, (i + step) % count) for i in range(count)])


def ring_step(stage, right, left):
    stage, right[-1], left[-1] = lax.optimization_barrier((stage, right[-1], left[-1]))
    right.append(hop(right[-1], 1))
    left.append(hop(left[-1], -1))
    return stage


def tile_columns(weight):
    rows, cols = weight.shape
    return weight.reshape(rows, cols // 128, 128).swapaxes(0, 1).reshape(-1, 128)


def regroup(tiles, rows):
    devices = tiles.shape[0]
    tiles = tiles.reshape(devices, -1, rows, 128).swapaxes(0, 1)
    return tiles.reshape(-1, 128)


def shards(
    latent_feats,
    conv_weight,
    kv_weight,
    stream,
    queries,
    norm_gain,
    up_weight,
    down_weight,
    band_start,
    band_end,
    visibility,
):
    view_id = lax.axis_index("view")
    core = view_id % 2
    first_row = lax.axis_index(SLAB) * 4
    where = jnp.stack([core, first_row, lax.axis_index("dp")]).astype(jnp.int32)
    feats = latent_feats[0, 0]
    ends = lax.axis_size(SLAB) - 1
    above = lax.ppermute(feats[2:], SLAB, [(i, i + 1) for i in range(ends)])
    below = lax.ppermute(feats[:2], SLAB, [(i + 1, i) for i in range(ends)])
    rows = jnp.concatenate([above, feats, below], axis=0).reshape(256, 256)

    conv_half = jnp.where(core == 0, conv_weight[:, :128], conv_weight[:, 128:])
    kv_half = jnp.where(
        core == 0,
        jnp.concatenate([kv_weight[:, :384], kv_weight[:, 768:1152]], axis=1),
        jnp.concatenate([kv_weight[:, 384:768], kv_weight[:, 1152:]], axis=1),
    )
    mine_code = jnp.concatenate([conv_half, tile_columns(kv_half)], axis=0)
    mine_units = jnp.concatenate([tile_columns(up_weight), tile_columns(down_weight)], axis=0)
    slabs = copy_for_each(mine_code, SLAB)
    slabs, rows, mine_units = lax.optimization_barrier((slabs, rows, mine_units))
    code = jnp.concatenate([regroup(slabs[:, :18], 18), regroup(slabs[:, 18:], 2)], axis=0)
    right, left = [code], [code]
    for _ in range(3):
        right.append(hop(right[-1], 1))
        left.append(hop(left[-1], -1))
    right.append(hop(right[-1], 1))
    own = jnp.stack(right + left[:0:-1])
    other = lax.ppermute(own, "view", [(i, i ^ 1) for i in range(4)])

    slabs = copy_for_each(mine_units, SLAB)
    units = jnp.concatenate([regroup(slabs[:, :36], 6), regroup(slabs[:, 36:], 6)], axis=0)
    right, left = [units, hop(units, 1)], [units, hop(units, -1)]

    encoded = kernel_call(
        conv_kernel,
        jax.ShapeDtypeStruct((192, 256), BF),
        [SMEM, VMEM, VMEM, VMEM],
        name="encode",
    )(where, rows, own, other)
    encoded = ring_step(encoded, right, left)
    nearby = lax.all_gather(encoded, "view", axis=0, tiled=True)
    nearby = ring_step(nearby, right, left)
    vis_row = lax.dynamic_index_in_dim(visibility[0], view_id, 0, False)
    seen = jnp.where(jnp.arange(4) == view_id, 1, vis_row).astype(jnp.int32)
    normed, residual = kernel_call(
        attention_kernel,
        (jax.ShapeDtypeStruct((128, 768), BF), jax.ShapeDtypeStruct((128, 768), F32)),
        [SMEM, SMEM, SMEM, SMEM] + [VMEM] * 6,
        scratch=[pltpu.VMEM((12, 768, 128), BF), pltpu.VMEM((128, 768), F32)],
        name="attend",
    )(
        where,
        band_start[0, 0],
        band_end[0, 0],
        seen,
        nearby,
        own,
        other,
        queries[0, 0].reshape(128, 768),
        stream[0, 0].reshape(128, 768),
        norm_gain.reshape(1, 768),
    )
    normed, upper, lower = lax.optimization_barrier((normed, right[3], left[3]))
    mlp = (*right[:3], upper, *left[1:3], lower, hop(upper[:576], 1), hop(lower[576:], -1))
    tokens = lax.all_gather(normed, "view", axis=0, tiled=True)
    parts = kernel_call(
        mlp_kernel,
        jax.ShapeDtypeStruct((4, 128, 768), BF),
        [SMEM] + [VMEM] * 10,
        scratch=[pltpu.VMEM((768, 768), BF), pltpu.VMEM((768, 768), BF)],
        name="mlp",
    )(where, tokens, *mlp)
    arrived = lax.all_to_all(parts, "view", split_axis=0, concat_axis=0, tiled=True)
    mixed = arrived.astype(F32).sum(axis=0)
    return (residual + mixed).astype(BF).reshape(1, 1, 4, 32, 768)


def solution(mesh):
    finer = Mesh(
        mesh.devices.reshape(mesh.shape["dp"], 2, 8, mesh.shape["view"]),
        ("dp", "slab_0", "slab_1", "view"),
    )
    in_specs = (
        P("dp", "view", SLAB, None, None),
        P(DP_SLAB, None),
        P(DP_SLAB, None),
        P("dp", "view", SLAB, None, None),
        P("dp", "view", SLAB, None, None),
        P(),
        P(DP_SLAB, "view"),
        P(DP_SLAB, "view"),
        P("dp", "view", SLAB, None),
        P("dp", "view", SLAB, None),
        P("dp", None, None),
    )
    out_specs = P("dp", "view", SLAB, None, None)
    return jax.shard_map(
        shards, mesh=finer, in_specs=in_specs, out_specs=out_specs, check_vma=False
    )
```

```python
import jax
import jax.numpy as jnp
import numpy as np
from jax import lax
from jax.experimental import pallas as pl
from jax.experimental.pallas import tpu as pltpu
from jax.sharding import Mesh
from jax.sharding import PartitionSpec as P

HEADS = 12
HEAD_DIM = 64
SLAB = ("slab_0", "slab_1")
DP_SLAB = ("dp", "slab_0", "slab_1")
BF = jnp.bfloat16
F32 = jnp.float32

VMEM = pl.BlockSpec(memory_space=pltpu.VMEM)
SMEM = pl.BlockSpec(memory_space=pltpu.SMEM)


def one_hot(size, rows):
    place = lax.broadcasted_iota(jnp.int32, (1, size), 1)
    z = place // (16 * rows)
    rest = place % (16 * rows)
    row = (rest // rows * 8 + z) * rows + rest % rows
    here = lax.broadcasted_iota(jnp.int32, (size, size), 0)
    return jnp.where(here == row, 1.0, 0.0).astype(BF)


def conv_kernel(where_ref, x_ref, own_ref, other_ref, out_ref):
    first = where_ref[0] == 0
    x = x_ref[...].astype(F32)
    col = lax.broadcasted_iota(jnp.int32, x.shape, 0) % 32
    left = jnp.where(col == 0, 0.0, pltpu.roll(x, 1, 0)).astype(BF)
    right = jnp.where(col == 31, 0.0, pltpu.roll(x, x.shape[0] - 1, 0)).astype(BF)
    shifted = (left, x_ref[...], right)
    tiles = []
    for tile in range(2):
        at = slice(tile * 288, (tile + 1) * 288)
        tiles.append(
            jnp.concatenate(
                [jnp.where(first, own_ref[d, at, :], other_ref[d, at, :]) for d in range(8)], axis=0
            )
        )
    weight = jnp.concatenate(tiles, axis=1)
    conv = jnp.zeros((192, 256), F32)
    for tap in range(9):
        rows = shifted[tap % 3][tap // 3 * 32 : tap // 3 * 32 + 192]
        conv = conv + jnp.dot(
            rows, weight[tap * 256 : (tap + 1) * 256], preferred_element_type=F32
        )
    silu = conv / (1.0 + jnp.exp(-conv))
    encoded = (x[32:224] + silu).astype(BF)
    out_ref[...] = jnp.dot(encoded, one_hot(256, 2), preferred_element_type=F32).astype(BF)


def attention_kernel(
    where_ref,
    start_ref,
    end_ref,
    seen_ref,
    enc_ref,
    own_ref,
    other_ref,
    q_ref,
    stream_ref,
    gain_ref,
    normed_ref,
    residual_ref,
    kv_ref,
    bias_ref,
):
    first = where_ref[0] == 0
    first_row = where_ref[1]
    enc = enc_ref[...]
    for tile in range(12):
        at = slice(tile * 32, (tile + 1) * 32)
        weight = jnp.concatenate(
            [jnp.where(first, other_ref[z, at, :], own_ref[z, at, :]) for z in range(8)], axis=0
        )
        kv_ref[tile] = jnp.dot(enc, weight, preferred_element_type=F32).astype(BF)
    lane = lax.broadcasted_iota(jnp.int32, (1, 768), 1)
    key_view = lane // 192
    key_row = first_row - 1 + (lane % 192) // 32
    for r in range(4):
        low = jnp.zeros((1, 768), jnp.int32)
        high = jnp.zeros((1, 768), jnp.int32)
        for u in range(4):
            mine = key_view == u
            low = jnp.where(mine, start_ref[r, u], low)
            high = jnp.where(mine, jnp.where(seen_ref[u] == 1, end_ref[r, u], -1), high)
        bias = jnp.where((low <= key_row) & (key_row < high), 0.0, -1e30)
        bias_ref[r * 32 : (r + 1) * 32, :] = jnp.broadcast_to(bias, (32, 768))
    left = lax.broadcasted_iota(jnp.int32, (128, 128), 1) < HEAD_DIM
    square = jnp.zeros((128, 1), F32)
    for pair in range(6):
        q = q_ref[:, pair * 128 : (pair + 1) * 128]
        zero = jnp.zeros_like(q)
        keys = kv_ref[pair]
        values = kv_ref[6 + pair]
        outs = []
        for side in range(2):
            mine = left if side == 0 else ~left
            scores = lax.dot_general(
                jnp.where(mine, q, zero), keys, (((1,), (1,)), ((), ())), preferred_element_type=F32
            )
            scores = scores * HEAD_DIM ** (-0.5) + bias_ref[...]
            weights = jnp.exp(scores - jnp.max(scores, axis=-1, keepdims=True))
            total = jnp.sum(weights, axis=-1, keepdims=True)
            probs = (weights / total).astype(BF)
            outs.append(jnp.dot(probs, values, preferred_element_type=F32))
        attended = jnp.where(left, outs[0], outs[1])
        cols = slice(pair * 128, (pair + 1) * 128)
        residual = stream_ref[:, cols].astype(F32) + attended
        residual_ref[:, cols] = residual
        square = square + jnp.sum(residual * residual, axis=-1, keepdims=True)
    scale = lax.rsqrt(square * (1.0 / 768) + 1e-6)
    normed_ref[...] = (residual_ref[...] * scale * gain_ref[...]).astype(BF)


def gelu(v):
    return 0.5 * v * (1.0 + jnp.tanh(0.7978845608028654 * (v + 0.044715 * (v * v * v))))


def mlp_kernel(where_ref, tok_ref, w_ref, out_ref, up_ref, down_ref):
    for tile in range(6):
        cols = slice(tile * 128, (tile + 1) * 128)
        for d in range(8):
            rows = slice(d * 96, (d + 1) * 96)
            up_ref[rows, cols] = w_ref[d, tile * 96 : (tile + 1) * 96, :]
            down_ref[rows, cols] = w_ref[d, 576 + tile * 96 : 576 + (tile + 1) * 96, :]

    def run(swap):
        for block in range(4):
            tokens = tok_ref[block * 128 : (block + 1) * 128, :]
            if swap is not None:
                tokens = jnp.dot(tokens, swap, preferred_element_type=F32).astype(BF)
            hidden = gelu(jnp.dot(tokens, up_ref[...], preferred_element_type=F32)).astype(BF)
            part = last_dims(hidden, down_ref[...])
            if swap is not None:
                part = last_dims(part, swap)
            out_ref[block] = part

    @pl.when(where_ref[0] == 0)
    def _():
        run(None)

    @pl.when(where_ref[0] != 0)
    def _():
        run(one_hot(768, 6))


def last_dims(a, b):
    return lax.dot_general(
        a, b, (((1,), (1,)), ((), ())), preferred_element_type=F32
    ).astype(BF)


def kernel_call(body, out_shape, in_specs, scratch=(), name=None):
    outs = jax.tree.map(lambda _: VMEM, out_shape)
    return pl.pallas_call(
        body,
        out_shape=out_shape,
        in_specs=in_specs,
        out_specs=outs,
        scratch_shapes=scratch,
        name=name,
        compiler_params=pltpu.CompilerParams(vmem_limit_bytes=16 << 20),
    )


def by_core(even, odd):
    ids = np.arange(512).reshape(8, 2, 8, 4)
    groups = []
    for axes, views in ((even, (0, 2)), (odd, (1, 3))):
        held = [axis for axis in range(3) if axis not in axes]
        for view in views:
            lines = ids[..., view].transpose(*held, *axes)
            groups.extend(lines.reshape(-1, int(np.prod([ids.shape[a] for a in axes]))).tolist())
    return groups


def copies_of(value, count):
    return jnp.broadcast_to(value, (count, *value.shape))


def exchange(copies, groups):
    return lax.all_to_all(
        copies,
        ("dp", "slab_0", "slab_1", "view"),
        split_axis=0,
        concat_axis=0,
        axis_index_groups=groups,
        tiled=True,
    )


def tile_columns(weight):
    rows, cols = weight.shape
    return weight.reshape(rows, cols // 128, 128).swapaxes(0, 1).reshape(-1, 128)


def regroup(tiles, rows):
    devices = tiles.shape[0]
    tiles = tiles.reshape(devices, -1, rows, 128).swapaxes(0, 1)
    return tiles.reshape(-1, 128)


def shards(
    latent_feats,
    conv_weight,
    kv_weight,
    stream,
    queries,
    norm_gain,
    up_weight,
    down_weight,
    band_start,
    band_end,
    visibility,
):
    view_id = lax.axis_index("view")
    core = view_id % 2
    first_row = lax.axis_index(SLAB) * 4
    where = jnp.stack([core, first_row]).astype(jnp.int32)
    feats = latent_feats[0, 0]
    ends = lax.axis_size(SLAB) - 1
    above = lax.ppermute(feats[2:], SLAB, [(i, i + 1) for i in range(ends)])
    below = lax.ppermute(feats[:2], SLAB, [(i + 1, i) for i in range(ends)])
    rows = jnp.concatenate([above, feats, below], axis=0).reshape(256, 256)

    even = core == 0
    code = jnp.where(
        even, tile_columns(conv_weight), jnp.pad(tile_columns(kv_weight), ((0, 12), (0, 0)))
    )
    mine = jnp.concatenate([code, tile_columns(up_weight), tile_columns(down_weight)], axis=0)
    wide = by_core((1, 2), (0, 1))
    long = by_core((0,), (2,))
    near = exchange(copies_of(mine, 16), wide)
    near, rows = lax.optimization_barrier((near, rows))
    code = jnp.where(
        even, regroup(near[:, :36], 18), jnp.pad(regroup(near[:, :24], 2), ((0, 192), (0, 0)))
    )
    units = jnp.concatenate([regroup(near[:, 36:72], 6), regroup(near[:, 72:], 6)], axis=0)
    own = exchange(copies_of(code, 8), long)
    units = copies_of(units, 8)
    own, units = lax.optimization_barrier((own, units))
    other = lax.ppermute(own, "view", [(i, i ^ 1) for i in range(4)])
    mlp = exchange(units, long)

    encoded = kernel_call(
        conv_kernel,
        jax.ShapeDtypeStruct((192, 256), BF),
        [SMEM, VMEM, VMEM, VMEM],
        name="encode",
    )(where, rows, own, other)
    nearby = lax.all_gather(encoded, "view", axis=0, tiled=True)
    vis_row = lax.dynamic_index_in_dim(visibility[0], view_id, 0, False)
    seen = jnp.where(jnp.arange(4) == view_id, 1, vis_row).astype(jnp.int32)
    normed, residual = kernel_call(
        attention_kernel,
        (jax.ShapeDtypeStruct((128, 768), BF), jax.ShapeDtypeStruct((128, 768), F32)),
        [SMEM, SMEM, SMEM, SMEM] + [VMEM] * 6,
        scratch=[pltpu.VMEM((12, 768, 128), BF), pltpu.VMEM((128, 768), F32)],
        name="attend",
    )(
        where,
        band_start[0, 0],
        band_end[0, 0],
        seen,
        nearby,
        own,
        other,
        queries[0, 0].reshape(128, 768),
        stream[0, 0].reshape(128, 768),
        norm_gain.reshape(1, 768),
    )
    tokens = lax.all_gather(normed, "view", axis=0, tiled=True)
    parts = kernel_call(
        mlp_kernel,
        jax.ShapeDtypeStruct((4, 128, 768), BF),
        [SMEM, VMEM, VMEM],
        scratch=[pltpu.VMEM((768, 768), BF), pltpu.VMEM((768, 768), BF)],
        name="mlp",
    )(where, tokens, mlp)
    arrived = lax.all_to_all(parts, "view", split_axis=0, concat_axis=0, tiled=True)
    mixed = arrived.astype(F32).sum(axis=0)
    return (residual + mixed).astype(BF).reshape(1, 1, 4, 32, 768)


def solution(mesh):
    finer = Mesh(
        mesh.devices.reshape(mesh.shape["dp"], 2, 8, mesh.shape["view"]),
        ("dp", "slab_0", "slab_1", "view"),
    )
    in_specs = (
        P("dp", "view", SLAB, None, None),
        P(DP_SLAB, None),
        P(DP_SLAB, None),
        P("dp", "view", SLAB, None, None),
        P("dp", "view", SLAB, None, None),
        P(),
        P(DP_SLAB, "view"),
        P(DP_SLAB, "view"),
        P("dp", "view", SLAB, None),
        P("dp", "view", SLAB, None),
        P("dp", None, None),
    )
    out_specs = P("dp", "view", SLAB, None, None)
    return jax.shard_map(
        shards, mesh=finer, in_specs=in_specs, out_specs=out_specs, check_vma=False
    )
```

```python
import jax
import jax.numpy as jnp
import numpy as np
from jax import lax
from jax.experimental import pallas as pl
from jax.experimental.pallas import tpu as pltpu
from jax.sharding import Mesh
from jax.sharding import PartitionSpec as P

HEAD_DIM = 64
SLAB = ("slab_0", "slab_1")
DP_SLAB = ("dp", "slab_0", "slab_1")
BF = jnp.bfloat16
F32 = jnp.float32

VMEM = pl.BlockSpec(memory_space=pltpu.VMEM)
HBM = pl.BlockSpec(memory_space=pltpu.HBM)
SMEM = pl.BlockSpec(memory_space=pltpu.SMEM)


def one_hot(size, rows):
    place = lax.broadcasted_iota(jnp.int32, (1, size), 1)
    z = place // (16 * rows)
    rest = place % (16 * rows)
    row = (rest // rows * 8 + z) * rows + rest % rows
    here = lax.broadcasted_iota(jnp.int32, (size, size), 0)
    return jnp.where(here == row, 1.0, 0.0).astype(BF)


def conv_kernel(where_ref, rows_ref, own_ref, other_ref, out_ref, x_ref, weight_ref, sem):
    copy = pltpu.make_async_copy(rows_ref, x_ref, sem)
    copy.start()
    for core, ref in ((0, own_ref), (1, other_ref)):

        @pl.when(where_ref[0] == core)
        def _(ref=ref):
            for tile in range(2):
                cols = slice(tile * 128, (tile + 1) * 128)
                for d in range(8):
                    rows = slice(d * 288, (d + 1) * 288)
                    weight_ref[rows, cols] = ref[d, tile * 288 : (tile + 1) * 288, :]

    copy.wait()
    x = x_ref[...].astype(F32)
    col = lax.broadcasted_iota(jnp.int32, x.shape, 0) % 32
    left = jnp.where(col == 0, 0.0, pltpu.roll(x, 1, 0)).astype(BF)
    right = jnp.where(col == 31, 0.0, pltpu.roll(x, x.shape[0] - 1, 0)).astype(BF)
    shifted = (left, x_ref[...], right)
    conv = jnp.zeros((192, 256), F32)
    for tap in range(9):
        rows = shifted[tap % 3][tap // 3 * 32 : tap // 3 * 32 + 192]
        conv = conv + jnp.dot(
            rows, weight_ref[tap * 256 : (tap + 1) * 256, :], preferred_element_type=F32
        )
    silu = conv / (1.0 + jnp.exp(-conv))
    encoded = (x[32:224] + silu).astype(BF)
    out_ref[...] = jnp.dot(encoded, one_hot(256, 2), preferred_element_type=F32).astype(BF)


def attention_kernel(
    where_ref,
    start_ref,
    end_ref,
    seen_ref,
    enc_ref,
    own_ref,
    other_ref,
    q_ref,
    stream_ref,
    gain_ref,
    normed_ref,
    far_ref,
    kv_ref,
    bias_ref,
    residual_ref,
    sems,
):
    first = where_ref[0] == 0
    first_row = where_ref[1]
    enc = enc_ref[...]
    for tile in range(12):
        at = slice(tile * 32, (tile + 1) * 32)
        weight = jnp.concatenate(
            [jnp.where(first, other_ref[z, at, :], own_ref[z, at, :]) for z in range(8)], axis=0
        )
        kv_ref[tile] = jnp.dot(enc, weight, preferred_element_type=F32).astype(BF)
    lane = lax.broadcasted_iota(jnp.int32, (1, 768), 1)
    key_view = lane // 192
    key_row = first_row - 1 + (lane % 192) // 32
    for r in range(4):
        low = jnp.zeros((1, 768), jnp.int32)
        high = jnp.zeros((1, 768), jnp.int32)
        for u in range(4):
            mine = key_view == u
            low = jnp.where(mine, start_ref[r, u], low)
            high = jnp.where(mine, jnp.where(seen_ref[u] == 1, end_ref[r, u], -1), high)
        bias = jnp.where((low <= key_row) & (key_row < high), 0.0, -1e30)
        bias_ref[r * 32 : (r + 1) * 32, :] = jnp.broadcast_to(bias, (32, 768))
    left = lax.broadcasted_iota(jnp.int32, (128, 128), 1) < HEAD_DIM
    square = jnp.zeros((128, 1), F32)
    copies = []
    for pair in range(6):
        q = q_ref[:, pair * 128 : (pair + 1) * 128]
        zero = jnp.zeros_like(q)
        keys = kv_ref[pair]
        values = kv_ref[6 + pair]
        both = jnp.concatenate([jnp.where(left, q, zero), jnp.where(left, zero, q)], axis=0)
        scores = lax.dot_general(
            both, keys, (((1,), (1,)), ((), ())), preferred_element_type=F32
        )
        bias = bias_ref[...]
        scores = scores * HEAD_DIM ** (-0.5) + jnp.concatenate([bias, bias], axis=0)
        weights = jnp.exp(scores - jnp.max(scores, axis=-1, keepdims=True))
        share = 1.0 / jnp.sum(weights, axis=-1, keepdims=True)
        outs = jnp.dot(weights.astype(BF), values, preferred_element_type=F32) * share
        attended = jnp.where(left, outs[:128], outs[128:])
        cols = slice(pair * 128, (pair + 1) * 128)
        residual = stream_ref[:, cols].astype(F32) + attended
        residual_ref[:, cols] = residual
        copies.append(
            pltpu.make_async_copy(residual_ref.at[:, cols], far_ref.at[:, cols], sems.at[pair])
        )
        copies[-1].start()
        square = square + jnp.sum(residual * residual, axis=-1, keepdims=True)
    scale = lax.rsqrt(square * (1.0 / 768) + 1e-6)
    normed_ref[...] = (residual_ref[...] * scale * gain_ref[...]).astype(BF)
    for copy in copies:
        copy.wait()


def gelu(v):
    return 0.5 * v * (1.0 + jnp.tanh(0.7978845608028654 * (v + 0.044715 * (v * v * v))))


def mlp_kernel(tok_ref, w_ref, out_ref, up_ref, down_ref):
    for tile in range(6):
        cols = slice(tile * 128, (tile + 1) * 128)
        for d in range(8):
            rows = slice(d * 96, (d + 1) * 96)
            up_ref[rows, cols] = w_ref[d, tile * 96 : (tile + 1) * 96, :]
            down_ref[rows, cols] = w_ref[d, 576 + tile * 96 : 576 + (tile + 1) * 96, :]

    for block in range(4):
        tokens = tok_ref[block * 128 : (block + 1) * 128, :]
        hidden = gelu(jnp.dot(tokens, up_ref[...], preferred_element_type=F32)).astype(BF)
        out_ref[block] = last_dims(hidden, down_ref[...]).astype(BF)


def swap_kernel(where_ref, tok_ref, out_ref):
    @pl.when(where_ref[0] == 0)
    def _():
        out_ref[...] = tok_ref[...]

    @pl.when(where_ref[0] != 0)
    def _():
        out_ref[...] = jnp.dot(tok_ref[...], one_hot(768, 6), preferred_element_type=F32).astype(BF)


def sum_kernel(parts_ref, residual_ref, out_ref):
    swap = one_hot(768, 6)
    odd = parts_ref[1].astype(F32) + parts_ref[3].astype(F32)
    high = odd.astype(BF)
    low = (odd - high.astype(F32)).astype(BF)
    odd = last_dims(high, swap) + last_dims(low, swap)
    even = parts_ref[0].astype(F32) + parts_ref[2].astype(F32)
    out_ref[...] = (residual_ref[...] + (even + odd)).astype(BF)


def last_dims(a, b):
    return lax.dot_general(a, b, (((1,), (1,)), ((), ())), preferred_element_type=F32)


def pack_kernel(where_ref, *refs):
    (sources, out_ref, held, sems) = (refs[:4], refs[4], refs[5:9], refs[9])
    copies = [pltpu.make_async_copy(sources[k], held[k], sems.at[k]) for k in range(4)]
    for copy in copies:
        copy.start()
    for copy in copies:
        copy.wait()
    conv_ref, kv_ref, up_ref, down_ref = held

    def tiles(ref, count):
        return [ref[:, t * 128 : (t + 1) * 128].astype(F32) for t in range(count)]

    mlp = tiles(up_ref, 6) + tiles(down_ref, 6)

    def put(code):
        block = jnp.concatenate(code + mlp, axis=0).astype(BF)
        for k in range(16):
            out_ref[k] = block

    @pl.when(where_ref[0] == 0)
    def _():
        put(tiles(conv_ref, 2))

    @pl.when(where_ref[0] != 0)
    def _():
        put(tiles(kv_ref, 12) + [jnp.zeros((12, 128), F32)])


def kernel_call(body, out_shape, in_specs, scratch=(), out_specs=None):
    outs = out_specs or jax.tree.map(lambda _: VMEM, out_shape)
    return pl.pallas_call(
        body,
        out_shape=out_shape,
        in_specs=in_specs,
        out_specs=outs,
        scratch_shapes=scratch,
        compiler_params=pltpu.CompilerParams(vmem_limit_bytes=16 << 20),
    )


def in_hbm(value):
    return pltpu.with_memory_space_constraint(value, pltpu.HBM)


def by_core(even, odd):
    ids = np.arange(512).reshape(8, 2, 8, 4)
    groups = []
    for axes, views in ((even, (0, 2)), (odd, (1, 3))):
        held = [axis for axis in range(3) if axis not in axes]
        for view in views:
            lines = ids[..., view].transpose(*held, *axes)
            groups.extend(lines.reshape(-1, int(np.prod([ids.shape[a] for a in axes]))).tolist())
    return groups


def copies_of(value, count):
    return jnp.broadcast_to(value, (count, *value.shape))


def exchange(copies, groups):
    return lax.all_to_all(
        copies,
        ("dp", "slab_0", "slab_1", "view"),
        split_axis=0,
        concat_axis=0,
        axis_index_groups=groups,
        tiled=True,
    )


def regroup(tiles, rows):
    devices = tiles.shape[0]
    tiles = tiles.reshape(devices, -1, rows, 128).swapaxes(0, 1)
    return tiles.reshape(-1, 128)


def shards(
    latent_feats,
    conv_weight,
    kv_weight,
    stream,
    queries,
    norm_gain,
    up_weight,
    down_weight,
    band_start,
    band_end,
    visibility,
):
    view_id = lax.axis_index("view")
    core = view_id % 2
    first_row = lax.axis_index(SLAB) * 4
    where = jnp.stack([core, first_row]).astype(jnp.int32)
    feats = latent_feats[0, 0]
    ends = lax.axis_size(SLAB) - 1
    above = lax.ppermute(feats[2:], SLAB, [(i, i + 1) for i in range(ends)])
    below = lax.ppermute(feats[:2], SLAB, [(i + 1, i) for i in range(ends)])
    rows = jnp.concatenate([above, feats, below], axis=0).reshape(256, 256)

    even = core == 0
    mine = kernel_call(
        pack_kernel,
        jax.ShapeDtypeStruct((16, 108, 128), BF),
        [SMEM] + [HBM] * 4,
        scratch=[pltpu.VMEM(w.shape, BF) for w in (conv_weight, kv_weight, up_weight, down_weight)]
        + [pltpu.SemaphoreType.DMA((4,))],
    )(where, *map(in_hbm, (conv_weight, kv_weight, up_weight, down_weight)))
    wide = by_core((1, 2), (0, 1))
    long = by_core((0,), (2,))
    near = exchange(mine, wide)
    near, rows = lax.optimization_barrier((near, rows))
    code = jnp.where(
        even, regroup(near[:, :36], 18), jnp.pad(regroup(near[:, :24], 2), ((0, 192), (0, 0)))
    )
    units = jnp.concatenate([regroup(near[:, 36:72], 6), regroup(near[:, 72:], 6)], axis=0)
    code = copies_of(code, 8)
    own = exchange(code, long)
    units = copies_of(units, 8)
    other = lax.ppermute(own, "view", [(i, i ^ 1) for i in range(4)])
    mlp = exchange(units, long)

    encoded = kernel_call(
        conv_kernel,
        jax.ShapeDtypeStruct((192, 256), BF),
        [SMEM, HBM, VMEM, VMEM],
        scratch=[
            pltpu.VMEM((256, 256), BF),
            pltpu.VMEM((2304, 256), BF),
            pltpu.SemaphoreType.DMA(()),
        ],
    )(where, in_hbm(rows), own, other)
    nearby = lax.all_gather(encoded, "view", axis=0, tiled=True)
    vis_row = lax.dynamic_index_in_dim(visibility[0], view_id, 0, False)
    seen = jnp.where(jnp.arange(4) == view_id, 1, vis_row).astype(jnp.int32)
    normed, residual = kernel_call(
        attention_kernel,
        (jax.ShapeDtypeStruct((128, 768), BF), pltpu.HBM((128, 768), F32)),
        [SMEM, SMEM, SMEM, SMEM] + [VMEM] * 6,
        scratch=[
            pltpu.VMEM((12, 768, 128), BF),
            pltpu.VMEM((128, 768), F32),
            pltpu.VMEM((128, 768), F32),
            pltpu.SemaphoreType.DMA((6,)),
        ],
        out_specs=(VMEM, HBM),
    )(
        where,
        band_start[0, 0],
        band_end[0, 0],
        seen,
        nearby,
        own,
        other,
        queries[0, 0].reshape(128, 768),
        stream[0, 0].reshape(128, 768),
        norm_gain.reshape(1, 768),
    )
    tokens = lax.all_gather(normed, "view", axis=0, tiled=True)
    tokens = kernel_call(
        swap_kernel, jax.ShapeDtypeStruct((512, 768), BF), [SMEM, VMEM]
    )(where, tokens)
    parts = kernel_call(
        mlp_kernel,
        jax.ShapeDtypeStruct((4, 128, 768), BF),
        [VMEM, VMEM],
        scratch=[pltpu.VMEM((768, 768), BF), pltpu.VMEM((768, 768), BF)],
    )(tokens, mlp)
    arrived = lax.all_to_all(parts, "view", split_axis=0, concat_axis=0, tiled=True)
    result = kernel_call(
        sum_kernel, jax.ShapeDtypeStruct((128, 768), BF), [VMEM] * 2
    )(arrived, residual)
    return result.reshape(1, 1, 4, 32, 768)


def solution(mesh):
    finer = Mesh(
        mesh.devices.reshape(mesh.shape["dp"], 2, 8, mesh.shape["view"]),
        ("dp", "slab_0", "slab_1", "view"),
    )
    in_specs = (
        P("dp", "view", SLAB, None, None),
        P(DP_SLAB, None),
        P(DP_SLAB, None),
        P("dp", "view", SLAB, None, None),
        P("dp", "view", SLAB, None, None),
        P(),
        P(DP_SLAB, "view"),
        P(DP_SLAB, "view"),
        P("dp", "view", SLAB, None),
        P("dp", "view", SLAB, None),
        P("dp", None, None),
    )
    out_specs = P("dp", "view", SLAB, None, None)
    return jax.shard_map(
        shards, mesh=finer, in_specs=in_specs, out_specs=out_specs, check_vma=False
    )
```

```python
import jax
import jax.numpy as jnp
import numpy as np
from jax import lax
from jax.experimental import pallas as pl
from jax.experimental.pallas import tpu as pltpu
from jax.sharding import Mesh
from jax.sharding import PartitionSpec as P

HEAD_DIM = 64
SLAB = ("slab_0", "slab_1")
DP_SLAB = ("dp", "slab_0", "slab_1")
BF = jnp.bfloat16
F32 = jnp.float32

VMEM = pl.BlockSpec(memory_space=pltpu.VMEM)
HBM = pl.BlockSpec(memory_space=pltpu.HBM)
SMEM = pl.BlockSpec(memory_space=pltpu.SMEM)


def one_hot(size, rows):
    place = lax.broadcasted_iota(jnp.int32, (1, size), 1)
    z = place // (16 * rows)
    rest = place % (16 * rows)
    row = (rest // rows * 8 + z) * rows + rest % rows
    here = lax.broadcasted_iota(jnp.int32, (size, size), 0)
    return jnp.where(here == row, 1.0, 0.0).astype(BF)


def conv_kernel(where_ref, rows_ref, own_ref, other_ref, out_ref, x_ref, sem):
    copy = pltpu.make_async_copy(rows_ref, x_ref, sem)
    copy.start()
    copy.wait()
    x = x_ref[...].astype(F32)
    col = lax.broadcasted_iota(jnp.int32, x.shape, 0) % 32
    left = jnp.where(col == 0, 0.0, pltpu.roll(x, 1, 0)).astype(BF)
    right = jnp.where(col == 31, 0.0, pltpu.roll(x, x.shape[0] - 1, 0)).astype(BF)
    shifted = (left, x_ref[...], right)
    swap = one_hot(256, 2)

    def tap_weight(ref, tap):
        tiles = []
        for tile in range(2):
            at, end, pieces = tap * 256, (tap + 1) * 256, []
            while at < end:
                d, low = divmod(at, 288)
                high = min(288, low + end - at)
                pieces.append(ref[d, tile * 288 + low : tile * 288 + high, :])
                at += high - low
            tiles.append(pieces[0] if len(pieces) == 1 else jnp.concatenate(pieces, axis=0))
        return jnp.concatenate(tiles, axis=1)

    for core, ref in ((0, own_ref), (1, other_ref)):

        @pl.when(where_ref[0] == core)
        def _(ref=ref):
            conv = jnp.zeros((192, 256), F32)
            for tap in range(9):
                rows = shifted[tap % 3][tap // 3 * 32 : tap // 3 * 32 + 192]
                conv = conv + jnp.dot(rows, tap_weight(ref, tap), preferred_element_type=F32)
            silu = conv / (1.0 + jnp.exp(-conv))
            encoded = (x[32:224] + silu).astype(BF)
            out_ref[...] = jnp.dot(encoded, swap, preferred_element_type=F32).astype(BF)


def attention_kernel(
    where_ref,
    start_ref,
    end_ref,
    seen_ref,
    enc_ref,
    own_ref,
    other_ref,
    q_ref,
    stream_ref,
    gain_ref,
    normed_ref,
    far_ref,
    kv_ref,
    bias_ref,
    residual_ref,
    sems,
):
    first = where_ref[0] == 0
    first_row = where_ref[1]
    enc = enc_ref[...]
    for couple in range(6):
        tiles = []
        for tile in (2 * couple, 2 * couple + 1):
            at = slice(tile * 32, (tile + 1) * 32)
            tiles.append(
                jnp.concatenate(
                    [jnp.where(first, other_ref[z, at, :], own_ref[z, at, :]) for z in range(8)],
                    axis=0,
                )
            )
        weight = jnp.concatenate(tiles, axis=1)
        kv = jnp.dot(enc, weight, preferred_element_type=F32).astype(BF)
        kv_ref[2 * couple] = kv[:, :128]
        kv_ref[2 * couple + 1] = kv[:, 128:]
    lane = lax.broadcasted_iota(jnp.int32, (1, 768), 1)
    key_view = lane // 192
    key_row = first_row - 1 + (lane % 192) // 32
    for r in range(4):
        low = jnp.zeros((1, 768), jnp.int32)
        high = jnp.zeros((1, 768), jnp.int32)
        for u in range(4):
            mine = key_view == u
            low = jnp.where(mine, start_ref[r, u], low)
            high = jnp.where(mine, jnp.where(seen_ref[u] == 1, end_ref[r, u], -1), high)
        bias = jnp.where((low <= key_row) & (key_row < high), 0.0, -1e30)
        bias_ref[r * 32 : (r + 1) * 32, :] = jnp.broadcast_to(bias, (32, 768))
    left = lax.broadcasted_iota(jnp.int32, (128, 128), 1) < HEAD_DIM
    square = jnp.zeros((128, 1), F32)
    copies = []
    for pair in range(6):
        q = q_ref[:, pair * 128 : (pair + 1) * 128]
        zero = jnp.zeros_like(q)
        keys = kv_ref[pair]
        values = kv_ref[6 + pair]
        both = jnp.concatenate([jnp.where(left, q, zero), jnp.where(left, zero, q)], axis=0)
        scores = lax.dot_general(
            both, keys, (((1,), (1,)), ((), ())), preferred_element_type=F32
        )
        bias = bias_ref[...]
        scores = scores * HEAD_DIM ** (-0.5) + jnp.concatenate([bias, bias], axis=0)
        weights = jnp.exp(scores - jnp.max(scores, axis=-1, keepdims=True))
        share = 1.0 / jnp.sum(weights, axis=-1, keepdims=True)
        outs = jnp.dot(weights.astype(BF), values, preferred_element_type=F32) * share
        attended = jnp.where(left, outs[:128], outs[128:])
        cols = slice(pair * 128, (pair + 1) * 128)
        residual = stream_ref[:, cols].astype(F32) + attended
        residual_ref[:, cols] = residual
        copies.append(
            pltpu.make_async_copy(residual_ref.at[:, cols], far_ref.at[:, cols], sems.at[pair])
        )
        copies[-1].start()
        square = square + jnp.sum(residual * residual, axis=-1, keepdims=True)
    scale = lax.rsqrt(square * (1.0 / 768) + 1e-6)
    normed_ref[...] = (residual_ref[...] * scale * gain_ref[...]).astype(BF)
    for copy in copies:
        copy.wait()


def gelu(v):
    return 0.5 * v * (1.0 + jnp.tanh(0.7978845608028654 * (v + 0.044715 * (v * v * v))))


def two_blocks(where_ref, tok_ref, up_ref, down_ref, out_refs, chip_flip):
    view = where_ref[2]
    for out_ref, flip in zip(out_refs, (0, 1)):
        rows = pl.ds(pl.multiple_of((view ^ (chip_flip * 2 + flip)) * 128, 128), 128)
        hidden = gelu(jnp.dot(tok_ref[rows, :], up_ref[...], preferred_element_type=F32)).astype(BF)
        out_ref[...] = last_dims(hidden, down_ref[...]).astype(BF)


def far_kernel(where_ref, tok_ref, w_ref, same_ref, cross_ref, up_ref, down_ref):
    for tile in range(6):
        cols = slice(tile * 128, (tile + 1) * 128)
        for d in range(8):
            rows = slice(d * 96, (d + 1) * 96)
            up_ref[rows, cols] = w_ref[d, tile * 96 : (tile + 1) * 96, :]
            down_ref[rows, cols] = w_ref[d, 576 + tile * 96 : 576 + (tile + 1) * 96, :]
    two_blocks(where_ref, tok_ref, up_ref, down_ref, (same_ref, cross_ref), 1)


def near_kernel(where_ref, tok_ref, up_ref, down_ref, own_ref, sibling_ref, swap_ref):
    two_blocks(where_ref, tok_ref, up_ref, down_ref, (own_ref, sibling_ref), 0)
    swap_ref[...] = one_hot(768, 6)


def swap_kernel(where_ref, tok_ref, out_ref):
    @pl.when(where_ref[0] == 0)
    def _():
        out_ref[...] = tok_ref[...]

    @pl.when(where_ref[0] != 0)
    def _():
        out_ref[...] = jnp.dot(tok_ref[...], one_hot(768, 6), preferred_element_type=F32).astype(BF)


def sum_kernel(
    where_ref, own_ref, sibling_ref, same_ref, cross_ref, swap_ref, residual_ref, out_ref
):
    alike = own_ref[...].astype(F32) + same_ref[...].astype(F32)
    unlike = sibling_ref[...].astype(F32) + cross_ref[...].astype(F32)
    first = where_ref[0] == 0
    odd = jnp.where(first, unlike, alike)
    even = jnp.where(first, alike, unlike)
    high = odd.astype(BF)
    low = (odd - high.astype(F32)).astype(BF)
    odd = last_dims(high, swap_ref[...]) + last_dims(low, swap_ref[...])
    out_ref[...] = (residual_ref[...] + (even + odd)).astype(BF)


def last_dims(a, b):
    return lax.dot_general(a, b, (((1,), (1,)), ((), ())), preferred_element_type=F32)


def pack_kernel(where_ref, *refs):
    (sources, out_ref, held, sems) = (refs[:4], refs[4], refs[5:9], refs[9])
    copies = [pltpu.make_async_copy(sources[k], held[k], sems.at[k]) for k in range(4)]
    for copy in copies:
        copy.start()
    for copy in copies:
        copy.wait()
    conv_ref, kv_ref, up_ref, down_ref = held

    def tiles(ref, count):
        return [ref[:, t * 128 : (t + 1) * 128].astype(F32) for t in range(count)]

    mlp = tiles(up_ref, 6) + tiles(down_ref, 6)

    def put(code):
        block = jnp.concatenate(code + mlp, axis=0).astype(BF)
        for k in range(16):
            out_ref[k] = block

    @pl.when(where_ref[0] == 0)
    def _():
        put(tiles(conv_ref, 2))

    @pl.when(where_ref[0] != 0)
    def _():
        put(tiles(kv_ref, 12) + [jnp.zeros((12, 128), F32)])


def kernel_call(body, out_shape, in_specs, scratch=(), out_specs=None):
    outs = out_specs or jax.tree.map(lambda _: VMEM, out_shape)
    return pl.pallas_call(
        body,
        out_shape=out_shape,
        in_specs=in_specs,
        out_specs=outs,
        scratch_shapes=scratch,
        compiler_params=pltpu.CompilerParams(vmem_limit_bytes=16 << 20),
    )


def in_hbm(value):
    return pltpu.with_memory_space_constraint(value, pltpu.HBM)


def by_core(even, odd):
    ids = np.arange(512).reshape(8, 2, 8, 4)
    groups = []
    for axes, views in ((even, (0, 2)), (odd, (1, 3))):
        held = [axis for axis in range(3) if axis not in axes]
        for view in views:
            lines = ids[..., view].transpose(*held, *axes)
            groups.extend(lines.reshape(-1, int(np.prod([ids.shape[a] for a in axes]))).tolist())
    return groups


def to_view(value, flip):
    return lax.ppermute(value, "view", [(i, i ^ flip) for i in range(4)])


def copies_of(value, count):
    return jnp.broadcast_to(value, (count, *value.shape))


def exchange(copies, groups):
    return lax.all_to_all(
        copies,
        ("dp", "slab_0", "slab_1", "view"),
        split_axis=0,
        concat_axis=0,
        axis_index_groups=groups,
        tiled=True,
    )


def regroup(tiles, rows):
    devices = tiles.shape[0]
    tiles = tiles.reshape(devices, -1, rows, 128).swapaxes(0, 1)
    return tiles.reshape(-1, 128)


def shards(
    latent_feats,
    conv_weight,
    kv_weight,
    stream,
    queries,
    norm_gain,
    up_weight,
    down_weight,
    band_start,
    band_end,
    visibility,
):
    view_id = lax.axis_index("view")
    core = view_id % 2
    first_row = lax.axis_index(SLAB) * 4
    where = jnp.stack([core, first_row, view_id]).astype(jnp.int32)
    feats = latent_feats[0, 0]
    ends = lax.axis_size(SLAB) - 1
    above = lax.ppermute(feats[2:], SLAB, [(i, i + 1) for i in range(ends)])
    below = lax.ppermute(feats[:2], SLAB, [(i + 1, i) for i in range(ends)])
    rows = jnp.concatenate([above, feats, below], axis=0).reshape(256, 256)

    even = core == 0
    mine = kernel_call(
        pack_kernel,
        jax.ShapeDtypeStruct((16, 108, 128), BF),
        [SMEM] + [HBM] * 4,
        scratch=[pltpu.VMEM(w.shape, BF) for w in (conv_weight, kv_weight, up_weight, down_weight)]
        + [pltpu.SemaphoreType.DMA((4,))],
    )(where, *map(in_hbm, (conv_weight, kv_weight, up_weight, down_weight)))
    wide = by_core((1, 2), (0, 1))
    long = by_core((0,), (2,))
    near = exchange(mine, wide)
    near, rows = lax.optimization_barrier((near, rows))
    code = jnp.where(
        even, regroup(near[:, :36], 18), jnp.pad(regroup(near[:, :24], 2), ((0, 192), (0, 0)))
    )
    units = jnp.concatenate([regroup(near[:, 36:72], 6), regroup(near[:, 72:], 6)], axis=0)
    code = copies_of(code, 8)
    own = exchange(code, long)
    units = copies_of(units, 8)
    other = to_view(own, 1)
    mlp = exchange(units, long)

    encoded = kernel_call(
        conv_kernel,
        jax.ShapeDtypeStruct((192, 256), BF),
        [SMEM, HBM, VMEM, VMEM],
        scratch=[
            pltpu.VMEM((256, 256), BF),
            pltpu.SemaphoreType.DMA(()),
        ],
    )(where, in_hbm(rows), own, other)
    nearby = lax.all_gather(encoded, "view", axis=0, tiled=True)
    vis_row = lax.dynamic_index_in_dim(visibility[0], view_id, 0, False)
    seen = jnp.where(jnp.arange(4) == view_id, 1, vis_row).astype(jnp.int32)
    normed, residual = kernel_call(
        attention_kernel,
        (jax.ShapeDtypeStruct((128, 768), BF), pltpu.HBM((128, 768), F32)),
        [SMEM, SMEM, SMEM, SMEM] + [VMEM] * 6,
        scratch=[
            pltpu.VMEM((12, 768, 128), BF),
            pltpu.VMEM((128, 768), F32),
            pltpu.VMEM((128, 768), F32),
            pltpu.SemaphoreType.DMA((6,)),
        ],
        out_specs=(VMEM, HBM),
    )(
        where,
        band_start[0, 0],
        band_end[0, 0],
        seen,
        nearby,
        own,
        other,
        queries[0, 0].reshape(128, 768),
        stream[0, 0].reshape(128, 768),
        norm_gain.reshape(1, 768),
    )
    tokens = lax.all_gather(normed, "view", axis=0, tiled=True)
    tokens = kernel_call(
        swap_kernel, jax.ShapeDtypeStruct((512, 768), BF), [SMEM, VMEM]
    )(where, tokens)
    block = jax.ShapeDtypeStruct((128, 768), BF)
    square = jax.ShapeDtypeStruct((768, 768), BF)
    same, cross, up, down = kernel_call(
        far_kernel, (block, block, square, square), [SMEM, VMEM, VMEM]
    )(where, tokens, mlp)
    cross = to_view(cross, 3)
    same = to_view(same, 2)
    own, sibling, swap = kernel_call(
        near_kernel, (block, block, square), [SMEM] + [VMEM] * 3
    )(where, tokens, up, down)
    sibling = to_view(sibling, 1)
    result = kernel_call(
        sum_kernel, block, [SMEM] + [VMEM] * 6
    )(where, own, sibling, same, cross, swap, residual)
    return result.reshape(1, 1, 4, 32, 768)


def solution(mesh):
    finer = Mesh(
        mesh.devices.reshape(mesh.shape["dp"], 2, 8, mesh.shape["view"]),
        ("dp", "slab_0", "slab_1", "view"),
    )
    in_specs = (
        P("dp", "view", SLAB, None, None),
        P(DP_SLAB, None),
        P(DP_SLAB, None),
        P("dp", "view", SLAB, None, None),
        P("dp", "view", SLAB, None, None),
        P(),
        P(DP_SLAB, "view"),
        P(DP_SLAB, "view"),
        P("dp", "view", SLAB, None),
        P("dp", "view", SLAB, None),
        P("dp", None, None),
    )
    out_specs = P("dp", "view", SLAB, None, None)
    return jax.shard_map(
        shards, mesh=finer, in_specs=in_specs, out_specs=out_specs, check_vma=False
    )
```

```python
import jax
import jax.numpy as jnp
import numpy as np
from jax import lax
from jax.experimental import pallas as pl
from jax.experimental.pallas import tpu as pltpu
from jax.sharding import Mesh
from jax.sharding import PartitionSpec as P

HEAD_DIM = 64
SLAB = ("slab_0", "slab_1")
DP_SLAB = ("dp", "slab_0", "slab_1")
BF = jnp.bfloat16
F32 = jnp.float32

VMEM = pl.BlockSpec(memory_space=pltpu.VMEM)
HBM = pl.BlockSpec(memory_space=pltpu.HBM)
SMEM = pl.BlockSpec(memory_space=pltpu.SMEM)


def one_hot(size, rows):
    place = lax.broadcasted_iota(jnp.int32, (1, size), 1)
    z = place // (16 * rows)
    rest = place % (16 * rows)
    row = (rest // rows * 8 + z) * rows + rest % rows
    here = lax.broadcasted_iota(jnp.int32, (size, size), 0)
    return jnp.where(here == row, 1.0, 0.0).astype(BF)


def conv_kernel(where_ref, rows_ref, own_ref, other_ref, out_ref, x_ref, sem):
    copy = pltpu.make_async_copy(rows_ref, x_ref, sem)
    copy.start()
    copy.wait()
    x = x_ref[...].astype(F32)
    col = lax.broadcasted_iota(jnp.int32, x.shape, 0) % 32
    left = jnp.where(col == 0, 0.0, pltpu.roll(x, 1, 0)).astype(BF)
    right = jnp.where(col == 31, 0.0, pltpu.roll(x, x.shape[0] - 1, 0)).astype(BF)
    shifted = (left, x_ref[...], right)
    swap = one_hot(256, 2)

    def tap_weight(ref, tap):
        tiles = []
        for tile in range(2):
            at, end, pieces = tap * 256, (tap + 1) * 256, []
            while at < end:
                d, low = divmod(at, 288)
                high = min(288, low + end - at)
                pieces.append(ref[d, tile * 288 + low : tile * 288 + high, :])
                at += high - low
            tiles.append(pieces[0] if len(pieces) == 1 else jnp.concatenate(pieces, axis=0))
        return jnp.concatenate(tiles, axis=1)

    for core, ref in ((0, own_ref), (1, other_ref)):

        @pl.when(where_ref[0] == core)
        def _(ref=ref):
            conv = jnp.zeros((192, 256), F32)
            for tap in range(9):
                rows = shifted[tap % 3][tap // 3 * 32 : tap // 3 * 32 + 192]
                conv = conv + jnp.dot(rows, tap_weight(ref, tap), preferred_element_type=F32)
            silu = conv / (1.0 + jnp.exp(-conv))
            encoded = (x[32:224] + silu).astype(BF)
            out_ref[...] = jnp.dot(encoded, swap, preferred_element_type=F32).astype(BF)


def attention_kernel(
    where_ref,
    start_ref,
    end_ref,
    seen_ref,
    enc_ref,
    own_ref,
    other_ref,
    q_ref,
    stream_ref,
    gain_ref,
    normed_ref,
    far_ref,
    kv_ref,
    bias_ref,
    residual_ref,
    sems,
):
    first = where_ref[0] == 0
    first_row = where_ref[1]
    enc = enc_ref[...]
    for couple in range(6):
        tiles = []
        for tile in (2 * couple, 2 * couple + 1):
            at = slice(tile * 32, (tile + 1) * 32)
            tiles.append(
                jnp.concatenate(
                    [jnp.where(first, other_ref[z, at, :], own_ref[z, at, :]) for z in range(8)],
                    axis=0,
                )
            )
        weight = jnp.concatenate(tiles, axis=1)
        kv = jnp.dot(enc, weight, preferred_element_type=F32).astype(BF)
        kv_ref[2 * couple] = kv[:, :128]
        kv_ref[2 * couple + 1] = kv[:, 128:]
    lane = lax.broadcasted_iota(jnp.int32, (1, 768), 1)
    key_view = lane // 192
    key_row = first_row - 1 + (lane % 192) // 32
    for r in range(4):
        low = jnp.zeros((1, 768), jnp.int32)
        high = jnp.zeros((1, 768), jnp.int32)
        for u in range(4):
            mine = key_view == u
            low = jnp.where(mine, start_ref[r, u], low)
            high = jnp.where(mine, jnp.where(seen_ref[u] == 1, end_ref[r, u], -1), high)
        bias = jnp.where((low <= key_row) & (key_row < high), 0.0, -1e30)
        bias_ref[r * 32 : (r + 1) * 32, :] = jnp.broadcast_to(bias, (32, 768))
    left = lax.broadcasted_iota(jnp.int32, (128, 128), 1) < HEAD_DIM
    square = jnp.zeros((128, 1), F32)
    copies = []
    for pair in range(6):
        q = q_ref[:, pair * 128 : (pair + 1) * 128]
        zero = jnp.zeros_like(q)
        keys = kv_ref[pair]
        values = kv_ref[6 + pair]
        both = jnp.concatenate([jnp.where(left, q, zero), jnp.where(left, zero, q)], axis=0)
        scores = lax.dot_general(
            both, keys, (((1,), (1,)), ((), ())), preferred_element_type=F32
        )
        bias = bias_ref[...]
        scores = scores * HEAD_DIM ** (-0.5) + jnp.concatenate([bias, bias], axis=0)
        weights = jnp.exp(scores - jnp.max(scores, axis=-1, keepdims=True))
        share = 1.0 / jnp.sum(weights, axis=-1, keepdims=True)
        outs = jnp.dot(weights.astype(BF), values, preferred_element_type=F32) * share
        attended = jnp.where(left, outs[:128], outs[128:])
        cols = slice(pair * 128, (pair + 1) * 128)
        residual = stream_ref[:, cols].astype(F32) + attended
        residual_ref[:, cols] = residual
        copies.append(
            pltpu.make_async_copy(residual_ref.at[:, cols], far_ref.at[:, cols], sems.at[pair])
        )
        copies[-1].start()
        square = square + jnp.sum(residual * residual, axis=-1, keepdims=True)
    scale = lax.rsqrt(square * (1.0 / 768) + 1e-6)
    normed_ref[...] = (residual_ref[...] * scale * gain_ref[...]).astype(BF)
    for copy in copies:
        copy.wait()


def gelu(v):
    return 0.5 * v * (1.0 + jnp.tanh(0.7978845608028654 * (v + 0.044715 * (v * v * v))))


def two_blocks(where_ref, tok_ref, w_ref, out_refs, chip_flip):
    blocks = []
    for flip in range(2):
        view = where_ref[2] ^ (chip_flip * 2 + flip)
        blocks.append(tok_ref[pl.ds(pl.multiple_of(view * 128, 128), 128), :])

    def gathered(at):
        tiles = []
        for tile in range(6):
            rows = slice(at + tile * 96, at + (tile + 1) * 96)
            tiles.append(jnp.concatenate([w_ref[d, rows, :] for d in range(8)], axis=0))
        return jnp.concatenate(tiles, axis=1)

    tokens = jnp.concatenate(blocks, axis=0)
    hidden = gelu(jnp.dot(tokens, gathered(0), preferred_element_type=F32)).astype(BF)
    parts = last_dims(hidden, gathered(576)).astype(BF)
    for k, out_ref in enumerate(out_refs):
        out_ref[...] = parts[k * 128 : (k + 1) * 128]


def far_kernel(where_ref, tok_ref, w_ref, same_ref, cross_ref):
    two_blocks(where_ref, tok_ref, w_ref, (same_ref, cross_ref), 1)


def near_kernel(where_ref, tok_ref, w_ref, own_ref, sibling_ref, swap_ref):
    two_blocks(where_ref, tok_ref, w_ref, (own_ref, sibling_ref), 0)
    swap_ref[...] = one_hot(768, 6)


def swap_kernel(where_ref, tok_ref, out_ref):
    @pl.when(where_ref[0] == 0)
    def _():
        out_ref[...] = tok_ref[...]

    @pl.when(where_ref[0] != 0)
    def _():
        out_ref[...] = jnp.dot(tok_ref[...], one_hot(768, 6), preferred_element_type=F32).astype(BF)


def sum_kernel(
    where_ref, own_ref, sibling_ref, same_ref, cross_ref, swap_ref, residual_ref, out_ref
):
    alike = own_ref[...].astype(F32) + same_ref[...].astype(F32)
    unlike = sibling_ref[...].astype(F32) + cross_ref[...].astype(F32)
    first = where_ref[0] == 0
    odd = jnp.where(first, unlike, alike)
    even = jnp.where(first, alike, unlike)
    high = odd.astype(BF)
    low = (odd - high.astype(F32)).astype(BF)
    both = last_dims(jnp.concatenate([high, low], axis=0), swap_ref[...])
    odd = both[:128] + both[128:]
    out_ref[...] = (residual_ref[...] + (even + odd)).astype(BF)


def last_dims(a, b):
    return lax.dot_general(a, b, (((1,), (1,)), ((), ())), preferred_element_type=F32)


def pack_kernel(where_ref, *refs):
    (sources, out_ref, held, sems) = (refs[:4], refs[4], refs[5:9], refs[9])
    copies = [pltpu.make_async_copy(sources[k], held[k], sems.at[k]) for k in range(4)]
    for copy in copies:
        copy.start()
    for copy in copies:
        copy.wait()
    conv_ref, kv_ref, up_ref, down_ref = held

    def tiles(ref, count):
        return [ref[:, t * 128 : (t + 1) * 128].astype(F32) for t in range(count)]

    mlp = tiles(up_ref, 6) + tiles(down_ref, 6)

    def put(code):
        block = jnp.concatenate(code + mlp, axis=0).astype(BF)
        for k in range(16):
            out_ref[k] = block

    @pl.when(where_ref[0] == 0)
    def _():
        put(tiles(conv_ref, 2))

    @pl.when(where_ref[0] != 0)
    def _():
        put(tiles(kv_ref, 12) + [jnp.zeros((12, 128), F32)])


def kernel_call(body, out_shape, in_specs, scratch=(), out_specs=None):
    outs = out_specs or jax.tree.map(lambda _: VMEM, out_shape)
    return pl.pallas_call(
        body,
        out_shape=out_shape,
        in_specs=in_specs,
        out_specs=outs,
        scratch_shapes=scratch,
        compiler_params=pltpu.CompilerParams(vmem_limit_bytes=16 << 20),
    )


def in_hbm(value):
    return pltpu.with_memory_space_constraint(value, pltpu.HBM)


def by_core(even, odd):
    ids = np.arange(512).reshape(8, 2, 8, 4)
    groups = []
    for axes, views in ((even, (0, 2)), (odd, (1, 3))):
        held = [axis for axis in range(3) if axis not in axes]
        for view in views:
            lines = ids[..., view].transpose(*held, *axes)
            groups.extend(lines.reshape(-1, int(np.prod([ids.shape[a] for a in axes]))).tolist())
    return groups


def to_view(value, flip):
    return lax.ppermute(value, "view", [(i, i ^ flip) for i in range(4)])


def copies_of(value, count):
    return jnp.broadcast_to(value, (count, *value.shape))


def exchange(copies, groups):
    return lax.all_to_all(
        copies,
        ("dp", "slab_0", "slab_1", "view"),
        split_axis=0,
        concat_axis=0,
        axis_index_groups=groups,
        tiled=True,
    )


def regroup(tiles, rows):
    devices = tiles.shape[0]
    tiles = tiles.reshape(devices, -1, rows, 128).swapaxes(0, 1)
    return tiles.reshape(-1, 128)


def shards(
    latent_feats,
    conv_weight,
    kv_weight,
    stream,
    queries,
    norm_gain,
    up_weight,
    down_weight,
    band_start,
    band_end,
    visibility,
):
    view_id = lax.axis_index("view")
    core = view_id % 2
    first_row = lax.axis_index(SLAB) * 4
    where = jnp.stack([core, first_row, view_id]).astype(jnp.int32)
    even = core == 0
    mine = kernel_call(
        pack_kernel,
        jax.ShapeDtypeStruct((16, 108, 128), BF),
        [SMEM] + [HBM] * 4,
        scratch=[pltpu.VMEM(w.shape, BF) for w in (conv_weight, kv_weight, up_weight, down_weight)]
        + [pltpu.SemaphoreType.DMA((4,))],
    )(where, *map(in_hbm, (conv_weight, kv_weight, up_weight, down_weight)))
    wide = by_core((1, 2), (0, 1))
    long = by_core((0,), (2,))
    near = exchange(mine, wide)
    near, feats = lax.optimization_barrier((near, latent_feats[0, 0]))
    ends = lax.axis_size(SLAB) - 1
    above = lax.ppermute(feats[2:], SLAB, [(i, i + 1) for i in range(ends)])
    below = lax.ppermute(feats[:2], SLAB, [(i + 1, i) for i in range(ends)])
    rows = jnp.concatenate([above, feats, below], axis=0).reshape(256, 256)
    code = jnp.where(
        even, regroup(near[:, :36], 18), jnp.pad(regroup(near[:, :24], 2), ((0, 192), (0, 0)))
    )
    units = jnp.concatenate([regroup(near[:, 36:72], 6), regroup(near[:, 72:], 6)], axis=0)
    code = copies_of(code, 8)
    own = exchange(code, long)
    units = copies_of(units, 8)
    other = to_view(own, 1)
    mlp = exchange(units, long)

    encoded = kernel_call(
        conv_kernel,
        jax.ShapeDtypeStruct((192, 256), BF),
        [SMEM, HBM, VMEM, VMEM],
        scratch=[
            pltpu.VMEM((256, 256), BF),
            pltpu.SemaphoreType.DMA(()),
        ],
    )(where, in_hbm(rows), own, other)
    nearby = lax.all_gather(encoded, "view", axis=0, tiled=True)
    vis_row = lax.dynamic_index_in_dim(visibility[0], view_id, 0, False)
    seen = jnp.where(jnp.arange(4) == view_id, 1, vis_row).astype(jnp.int32)
    normed, residual = kernel_call(
        attention_kernel,
        (jax.ShapeDtypeStruct((128, 768), BF), pltpu.HBM((128, 768), F32)),
        [SMEM, SMEM, SMEM, SMEM] + [VMEM] * 6,
        scratch=[
            pltpu.VMEM((12, 768, 128), BF),
            pltpu.VMEM((128, 768), F32),
            pltpu.VMEM((128, 768), F32),
            pltpu.SemaphoreType.DMA((6,)),
        ],
        out_specs=(VMEM, HBM),
    )(
        where,
        band_start[0, 0],
        band_end[0, 0],
        seen,
        nearby,
        own,
        other,
        queries[0, 0].reshape(128, 768),
        stream[0, 0].reshape(128, 768),
        norm_gain.reshape(1, 768),
    )
    tokens = lax.all_gather(normed, "view", axis=0, tiled=True)
    tokens = kernel_call(
        swap_kernel, jax.ShapeDtypeStruct((512, 768), BF), [SMEM, VMEM]
    )(where, tokens)
    block = jax.ShapeDtypeStruct((128, 768), BF)
    square = jax.ShapeDtypeStruct((768, 768), BF)
    same, cross = kernel_call(far_kernel, (block, block), [SMEM, VMEM, VMEM])(where, tokens, mlp)
    cross = to_view(cross, 3)
    same = to_view(same, 2)
    own, sibling, swap = kernel_call(
        near_kernel, (block, block, square), [SMEM, VMEM, VMEM]
    )(where, tokens, mlp)
    sibling = to_view(sibling, 1)
    result = kernel_call(
        sum_kernel, block, [SMEM] + [VMEM] * 6
    )(where, own, sibling, same, cross, swap, residual)
    return result.reshape(1, 1, 4, 32, 768)


def solution(mesh):
    finer = Mesh(
        mesh.devices.reshape(mesh.shape["dp"], 2, 8, mesh.shape["view"]),
        ("dp", "slab_0", "slab_1", "view"),
    )
    in_specs = (
        P("dp", "view", SLAB, None, None),
        P(DP_SLAB, None),
        P(DP_SLAB, None),
        P("dp", "view", SLAB, None, None),
        P("dp", "view", SLAB, None, None),
        P(),
        P(DP_SLAB, "view"),
        P(DP_SLAB, "view"),
        P("dp", "view", SLAB, None),
        P("dp", "view", SLAB, None),
        P("dp", None, None),
    )
    out_specs = P("dp", "view", SLAB, None, None)
    return jax.shard_map(
        shards, mesh=finer, in_specs=in_specs, out_specs=out_specs, check_vma=False
    )
```

```python
import jax
import jax.numpy as jnp
import numpy as np
from jax import lax
from jax.experimental import pallas as pl
from jax.experimental.pallas import tpu as pltpu
from jax.sharding import Mesh
from jax.sharding import PartitionSpec as P

HEAD_DIM = 64
SLAB = ("slab_0", "slab_1")
DP_SLAB = ("dp", "slab_0", "slab_1")
BF = jnp.bfloat16
F32 = jnp.float32

VMEM = pl.BlockSpec(memory_space=pltpu.VMEM)
HBM = pl.BlockSpec(memory_space=pltpu.HBM)
SMEM = pl.BlockSpec(memory_space=pltpu.SMEM)


def one_hot(size, rows):
    place = lax.broadcasted_iota(jnp.int32, (1, size), 1)
    z = place // (16 * rows)
    rest = place % (16 * rows)
    row = (rest // rows * 8 + z) * rows + rest % rows
    here = lax.broadcasted_iota(jnp.int32, (size, size), 0)
    return jnp.where(here == row, 1.0, 0.0).astype(BF)


def conv_kernel(where_ref, rows_ref, own_ref, other_ref, out_ref, x_ref, sem):
    copy = pltpu.make_async_copy(rows_ref, x_ref, sem)
    copy.start()
    copy.wait()
    lower = (where_ref[2] >> 1) == 0
    shifted, feats = [], []
    for k in range(2):
        rows = x_ref[k * 256 : (k + 1) * 256, :]
        x = rows.astype(F32)
        col = lax.broadcasted_iota(jnp.int32, x.shape, 0) % 32
        left = jnp.where(col == 0, 0.0, pltpu.roll(x, 1, 0)).astype(BF)
        right = jnp.where(col == 31, 0.0, pltpu.roll(x, x.shape[0] - 1, 0)).astype(BF)
        shifted.append((left, rows, right))
        feats.append(jnp.where(lower, x[32:224, :128], x[32:224, 128:]))
    feats = jnp.concatenate(feats, axis=0)

    def tap_weight(ref, tap):
        at, end, pieces = tap * 256, (tap + 1) * 256, []
        while at < end:
            d, low = divmod(at, 288)
            high = min(288, low + end - at)
            pieces.append(ref[d, low:high, :])
            at += high - low
        return pieces[0] if len(pieces) == 1 else jnp.concatenate(pieces, axis=0)

    for core, ref in ((0, own_ref), (1, other_ref)):

        @pl.when(where_ref[0] == core)
        def _(ref=ref):
            conv = jnp.zeros((384, 128), F32)
            for tap in range(9):
                at = slice(tap // 3 * 32, tap // 3 * 32 + 192)
                rows = jnp.concatenate([views[tap % 3][at] for views in shifted], axis=0)
                conv = conv + jnp.dot(rows, tap_weight(ref, tap), preferred_element_type=F32)
            silu = conv / (1.0 + jnp.exp(-conv))
            out_ref[...] = (feats + silu).astype(BF)


def attention_kernel(
    where_ref,
    start_ref,
    end_ref,
    seen_ref,
    enc_ref,
    own_ref,
    other_ref,
    q_ref,
    stream_ref,
    gain_ref,
    normed_ref,
    far_ref,
    kv_ref,
    bias_ref,
    residual_ref,
    sems,
):
    first = where_ref[0] == 0
    first_row = where_ref[1]
    enc = []
    for view in range(4):
        tiles = []
        for tile in range(2):
            device = tile * 2 + view % 2
            at = device * 384 + (0 if device == view else 192)
            tiles.append(enc_ref[at : at + 192, :])
        enc.append(jnp.concatenate(tiles, axis=1))
    enc = jnp.concatenate(enc, axis=0)
    enc = jnp.dot(enc, one_hot(256, 2), preferred_element_type=F32).astype(BF)
    for couple in range(6):
        tiles = []
        for tile in (2 * couple, 2 * couple + 1):
            at = slice(tile * 32, (tile + 1) * 32)
            tiles.append(
                jnp.concatenate(
                    [jnp.where(first, other_ref[z, at, :], own_ref[z, at, :]) for z in range(8)],
                    axis=0,
                )
            )
        weight = jnp.concatenate(tiles, axis=1)
        kv = jnp.dot(enc, weight, preferred_element_type=F32).astype(BF)
        kv_ref[2 * couple] = kv[:, :128]
        kv_ref[2 * couple + 1] = kv[:, 128:]
    lane = lax.broadcasted_iota(jnp.int32, (1, 768), 1)
    key_view = lane // 192
    key_row = first_row - 1 + (lane % 192) // 32
    for r in range(4):
        low = jnp.zeros((1, 768), jnp.int32)
        high = jnp.zeros((1, 768), jnp.int32)
        for u in range(4):
            mine = key_view == u
            low = jnp.where(mine, start_ref[r, u], low)
            high = jnp.where(mine, jnp.where(seen_ref[u] == 1, end_ref[r, u], -1), high)
        bias = jnp.where((low <= key_row) & (key_row < high), 0.0, -1e30)
        bias_ref[r * 32 : (r + 1) * 32, :] = jnp.broadcast_to(bias, (32, 768))
    left = lax.broadcasted_iota(jnp.int32, (128, 128), 1) < HEAD_DIM
    square = jnp.zeros((128, 1), F32)
    copies = []
    for pair in range(6):
        q = q_ref[:, pair * 128 : (pair + 1) * 128]
        zero = jnp.zeros_like(q)
        keys = kv_ref[pair]
        values = kv_ref[6 + pair]
        both = jnp.concatenate([jnp.where(left, q, zero), jnp.where(left, zero, q)], axis=0)
        scores = lax.dot_general(
            both, keys, (((1,), (1,)), ((), ())), preferred_element_type=F32
        )
        bias = bias_ref[...]
        scores = scores * HEAD_DIM ** (-0.5) + jnp.concatenate([bias, bias], axis=0)
        weights = jnp.exp(scores - jnp.max(scores, axis=-1, keepdims=True))
        share = 1.0 / jnp.sum(weights, axis=-1, keepdims=True)
        outs = jnp.dot(weights.astype(BF), values, preferred_element_type=F32) * share
        attended = jnp.where(left, outs[:128], outs[128:])
        cols = slice(pair * 128, (pair + 1) * 128)
        residual = stream_ref[:, cols].astype(F32) + attended
        residual_ref[:, cols] = residual
        copies.append(
            pltpu.make_async_copy(residual_ref.at[:, cols], far_ref.at[:, cols], sems.at[pair])
        )
        copies[-1].start()
        square = square + jnp.sum(residual * residual, axis=-1, keepdims=True)
    scale = lax.rsqrt(square * (1.0 / 768) + 1e-6)
    normed_ref[...] = (residual_ref[...] * scale * gain_ref[...]).astype(BF)
    for copy in copies:
        copy.wait()


def gelu(v):
    return 0.5 * v * (1.0 + jnp.tanh(0.7978845608028654 * (v + 0.044715 * (v * v * v))))


def blocks_of(where_ref, tok_ref, w_ref, out_refs, chip_flip, flips):
    blocks = []
    for flip in flips:
        view = where_ref[2] ^ (chip_flip * 2 + flip)
        blocks.append(tok_ref[pl.ds(pl.multiple_of(view * 128, 128), 128), :])

    def gathered(at):
        tiles = []
        for tile in range(6):
            rows = slice(at + tile * 96, at + (tile + 1) * 96)
            tiles.append(jnp.concatenate([w_ref[d, rows, :] for d in range(8)], axis=0))
        return jnp.concatenate(tiles, axis=1)

    tokens = jnp.concatenate(blocks, axis=0)
    hidden = gelu(jnp.dot(tokens, gathered(0), preferred_element_type=F32)).astype(BF)
    parts = last_dims(hidden, gathered(576)).astype(BF)
    for k, out_ref in enumerate(out_refs):
        out_ref[...] = parts[k * 128 : (k + 1) * 128]


def cross_kernel(where_ref, tok_ref, w_ref, cross_ref):
    blocks_of(where_ref, tok_ref, w_ref, (cross_ref,), 1, (1,))


def same_kernel(where_ref, tok_ref, w_ref, same_ref):
    blocks_of(where_ref, tok_ref, w_ref, (same_ref,), 1, (0,))


def near_kernel(where_ref, tok_ref, w_ref, own_ref, sibling_ref, swap_ref):
    blocks_of(where_ref, tok_ref, w_ref, (own_ref, sibling_ref), 0, (0, 1))
    swap_ref[...] = one_hot(768, 6)


def swap_kernel(where_ref, tok_ref, out_ref):
    @pl.when(where_ref[0] == 0)
    def _():
        out_ref[...] = tok_ref[...]

    @pl.when(where_ref[0] != 0)
    def _():
        out_ref[...] = jnp.dot(tok_ref[...], one_hot(768, 6), preferred_element_type=F32).astype(BF)


def sum_kernel(
    where_ref, own_ref, sibling_ref, same_ref, cross_ref, swap_ref, residual_ref, out_ref
):
    alike = own_ref[...].astype(F32) + same_ref[...].astype(F32)
    unlike = sibling_ref[...].astype(F32) + cross_ref[...].astype(F32)
    first = where_ref[0] == 0
    odd = jnp.where(first, unlike, alike)
    even = jnp.where(first, alike, unlike)
    high = odd.astype(BF)
    low = (odd - high.astype(F32)).astype(BF)
    both = last_dims(jnp.concatenate([high, low], axis=0), swap_ref[...])
    odd = both[:128] + both[128:]
    out_ref[...] = (residual_ref[...] + (even + odd)).astype(BF)


def last_dims(a, b):
    return lax.dot_general(a, b, (((1,), (1,)), ((), ())), preferred_element_type=F32)


def pack_kernel(where_ref, *refs):
    (sources, out_ref, held, sems) = (refs[:4], refs[4], refs[5:9], refs[9])
    copies = [pltpu.make_async_copy(sources[k], held[k], sems.at[k]) for k in range(4)]
    for copy in copies:
        copy.start()
    for copy in copies:
        copy.wait()
    conv_ref, kv_ref, up_ref, down_ref = held

    def tiles(ref, count):
        return [ref[:, t * 128 : (t + 1) * 128].astype(F32) for t in range(count)]

    mlp = tiles(up_ref, 6) + tiles(down_ref, 6)

    def put(code):
        block = jnp.concatenate(code + mlp, axis=0).astype(BF)
        for k in range(16):
            out_ref[k] = block

    @pl.when(where_ref[0] == 0)
    def _():
        low, high = tiles(conv_ref, 2)
        half = jnp.where((where_ref[2] >> 1) == 0, low, high)
        put([half, jnp.zeros((6, 128), F32)])

    @pl.when(where_ref[0] != 0)
    def _():
        put(tiles(kv_ref, 12))


def kernel_call(body, out_shape, in_specs, scratch=(), out_specs=None):
    outs = out_specs or jax.tree.map(lambda _: VMEM, out_shape)
    return pl.pallas_call(
        body,
        out_shape=out_shape,
        in_specs=in_specs,
        out_specs=outs,
        scratch_shapes=scratch,
        compiler_params=pltpu.CompilerParams(vmem_limit_bytes=16 << 20),
    )


def in_hbm(value):
    return pltpu.with_memory_space_constraint(value, pltpu.HBM)


def by_core(even, odd):
    ids = np.arange(512).reshape(8, 2, 8, 4)
    groups = []
    for axes, views in ((even, (1, 3)), (odd, (0, 2))):
        held = [axis for axis in range(3) if axis not in axes]
        for view in views:
            lines = ids[..., view].transpose(*held, *axes)
            groups.extend(lines.reshape(-1, int(np.prod([ids.shape[a] for a in axes]))).tolist())
    return groups


def to_view(value, flip):
    return lax.ppermute(value, "view", [(i, i ^ flip) for i in range(4)])


def copies_of(value, count):
    return jnp.broadcast_to(value, (count, *value.shape))


def exchange(copies, groups):
    return lax.all_to_all(
        copies,
        ("dp", "slab_0", "slab_1", "view"),
        split_axis=0,
        concat_axis=0,
        axis_index_groups=groups,
        tiled=True,
    )


def regroup(tiles, rows):
    devices = tiles.shape[0]
    tiles = tiles.reshape(devices, -1, rows, 128).swapaxes(0, 1)
    return tiles.reshape(-1, 128)


def shards(
    latent_feats,
    conv_weight,
    kv_weight,
    stream,
    queries,
    norm_gain,
    up_weight,
    down_weight,
    band_start,
    band_end,
    visibility,
):
    view_id = lax.axis_index("view")
    core = 1 - view_id % 2
    first_row = lax.axis_index(SLAB) * 4
    where = jnp.stack([core, first_row, view_id]).astype(jnp.int32)
    feats = latent_feats[0, 0]
    ends = lax.axis_size(SLAB) - 1
    above = lax.ppermute(feats[2:], SLAB, [(i, i + 1) for i in range(ends)])
    below = lax.ppermute(feats[:2], SLAB, [(i + 1, i) for i in range(ends)])
    rows = jnp.concatenate([above, feats, below], axis=0).reshape(256, 256)
    even = core == 0
    mine = kernel_call(
        pack_kernel,
        jax.ShapeDtypeStruct((16, 96, 128), BF),
        [SMEM] + [HBM] * 4,
        scratch=[pltpu.VMEM(w.shape, BF) for w in (conv_weight, kv_weight, up_weight, down_weight)]
        + [pltpu.SemaphoreType.DMA((4,))],
    )(where, *map(in_hbm, (conv_weight, kv_weight, up_weight, down_weight)))
    wide = by_core((1, 2), (0, 1))
    long = by_core((0,), (2,))
    near = exchange(mine, wide)
    near, rows = lax.optimization_barrier((near, rows))
    code = jnp.where(
        even, jnp.pad(regroup(near[:, :18], 18), ((0, 96), (0, 0))), regroup(near[:, :24], 2)
    )
    units = jnp.concatenate([regroup(near[:, 24:60], 6), regroup(near[:, 60:], 6)], axis=0)
    code = copies_of(code, 8)
    own = exchange(code, long)
    rows = jnp.concatenate([rows, to_view(rows, 2)], axis=0)
    units = copies_of(units, 8)
    other = to_view(own, 1)
    mlp = exchange(units, long)

    encoded = kernel_call(
        conv_kernel,
        jax.ShapeDtypeStruct((384, 128), BF),
        [SMEM, HBM, VMEM, VMEM],
        scratch=[
            pltpu.VMEM((512, 256), BF),
            pltpu.SemaphoreType.DMA(()),
        ],
    )(where, in_hbm(rows), own, other)
    nearby = lax.all_gather(encoded, "view", axis=0, tiled=True)
    vis_row = lax.dynamic_index_in_dim(visibility[0], view_id, 0, False)
    seen = jnp.where(jnp.arange(4) == view_id, 1, vis_row).astype(jnp.int32)
    normed, residual = kernel_call(
        attention_kernel,
        (jax.ShapeDtypeStruct((128, 768), BF), pltpu.HBM((128, 768), F32)),
        [SMEM, SMEM, SMEM, SMEM] + [VMEM] * 6,
        scratch=[
            pltpu.VMEM((12, 768, 128), BF),
            pltpu.VMEM((128, 768), F32),
            pltpu.VMEM((128, 768), F32),
            pltpu.SemaphoreType.DMA((6,)),
        ],
        out_specs=(VMEM, HBM),
    )(
        where,
        band_start[0, 0],
        band_end[0, 0],
        seen,
        nearby,
        own,
        other,
        queries[0, 0].reshape(128, 768),
        stream[0, 0].reshape(128, 768),
        norm_gain.reshape(1, 768),
    )
    tokens = lax.all_gather(normed, "view", axis=0, tiled=True)
    tokens = kernel_call(
        swap_kernel, jax.ShapeDtypeStruct((512, 768), BF), [SMEM, VMEM]
    )(where, tokens)
    block = jax.ShapeDtypeStruct((128, 768), BF)
    square = jax.ShapeDtypeStruct((768, 768), BF)
    cross = kernel_call(cross_kernel, block, [SMEM, VMEM, VMEM])(where, tokens, mlp)
    cross = to_view(cross, 3)
    same = kernel_call(same_kernel, block, [SMEM, VMEM, VMEM])(where, tokens, mlp)
    same = to_view(same, 2)
    own, sibling, swap = kernel_call(
        near_kernel, (block, block, square), [SMEM, VMEM, VMEM]
    )(where, tokens, mlp)
    sibling = to_view(sibling, 1)
    result = kernel_call(
        sum_kernel, block, [SMEM] + [VMEM] * 6
    )(where, own, sibling, same, cross, swap, residual)
    return result.reshape(1, 1, 4, 32, 768)


def solution(mesh):
    finer = Mesh(
        mesh.devices.reshape(mesh.shape["dp"], 2, 8, mesh.shape["view"]),
        ("dp", "slab_0", "slab_1", "view"),
    )
    in_specs = (
        P("dp", "view", SLAB, None, None),
        P(DP_SLAB, None),
        P(DP_SLAB, None),
        P("dp", "view", SLAB, None, None),
        P("dp", "view", SLAB, None, None),
        P(),
        P(DP_SLAB, "view"),
        P(DP_SLAB, "view"),
        P("dp", "view", SLAB, None),
        P("dp", "view", SLAB, None),
        P("dp", None, None),
    )
    out_specs = P("dp", "view", SLAB, None, None)
    return jax.shard_map(
        shards, mesh=finer, in_specs=in_specs, out_specs=out_specs, check_vma=False
    )
```

```python
import jax
import jax.numpy as jnp
import numpy as np
from jax import lax
from jax.experimental import pallas as pl
from jax.experimental.pallas import tpu as pltpu
from jax.sharding import Mesh
from jax.sharding import PartitionSpec as P

HEAD_DIM = 64
SLAB = ("slab_0", "slab_1")
DP_SLAB = ("dp", "slab_0", "slab_1")
BF = jnp.bfloat16
F32 = jnp.float32

VMEM = pl.BlockSpec(memory_space=pltpu.VMEM)
HBM = pl.BlockSpec(memory_space=pltpu.HBM)
SMEM = pl.BlockSpec(memory_space=pltpu.SMEM)


def one_hot(size, rows):
    place = lax.broadcasted_iota(jnp.int32, (1, size), 1)
    z = place // (16 * rows)
    rest = place % (16 * rows)
    row = (rest // rows * 8 + z) * rows + rest % rows
    here = lax.broadcasted_iota(jnp.int32, (size, size), 0)
    return jnp.where(here == row, 1.0, 0.0).astype(BF)


def conv_kernel(where_ref, rows_ref, own_ref, other_ref, out_ref, x_ref, sem):
    copy = pltpu.make_async_copy(rows_ref, x_ref, sem)
    copy.start()
    copy.wait()
    lower = (where_ref[2] >> 1) == 0
    shifted, feats = [], []
    for k in range(2):
        rows = x_ref[k * 256 : (k + 1) * 256, :]
        x = rows.astype(F32)
        col = lax.broadcasted_iota(jnp.int32, x.shape, 0) % 32
        left = jnp.where(col == 0, 0.0, pltpu.roll(x, 1, 0)).astype(BF)
        right = jnp.where(col == 31, 0.0, pltpu.roll(x, x.shape[0] - 1, 0)).astype(BF)
        shifted.append((left, rows, right))
        feats.append(jnp.where(lower, x[32:224, :128], x[32:224, 128:]))
    feats = jnp.concatenate(feats, axis=0)

    def tap_weight(ref, tap):
        at, end, pieces = tap * 256, (tap + 1) * 256, []
        while at < end:
            d, low = divmod(at, 288)
            high = min(288, low + end - at)
            pieces.append(ref[d, low:high, :])
            at += high - low
        return pieces[0] if len(pieces) == 1 else jnp.concatenate(pieces, axis=0)

    for core, ref in ((0, own_ref), (1, other_ref)):

        @pl.when(where_ref[0] == core)
        def _(ref=ref):
            conv = jnp.zeros((384, 128), F32)
            for tap in range(9):
                at = slice(tap // 3 * 32, tap // 3 * 32 + 192)
                rows = jnp.concatenate([views[tap % 3][at] for views in shifted], axis=0)
                conv = conv + jnp.dot(rows, tap_weight(ref, tap), preferred_element_type=F32)
            silu = conv / (1.0 + jnp.exp(-conv))
            out_ref[...] = (feats + silu).astype(BF)


def attention_kernel(
    where_ref,
    start_ref,
    end_ref,
    seen_ref,
    enc_ref,
    own_ref,
    other_ref,
    q_ref,
    stream_ref,
    gain_ref,
    normed_ref,
    far_ref,
    kv_ref,
    bias_ref,
    residual_ref,
    sems,
):
    first = where_ref[0] == 0
    first_row = where_ref[1]
    enc = []
    for view in range(4):
        tiles = []
        for tile in range(2):
            device = tile * 2 + view % 2
            at = device * 384 + (0 if device == view else 192)
            tiles.append(enc_ref[at : at + 192, :])
        enc.append(jnp.concatenate(tiles, axis=1))
    enc = jnp.concatenate(enc, axis=0)
    enc = jnp.dot(enc, one_hot(256, 2), preferred_element_type=F32).astype(BF)
    for couple in range(6):
        tiles = []
        for tile in (2 * couple, 2 * couple + 1):
            at = slice(tile * 32, (tile + 1) * 32)
            tiles.append(
                jnp.concatenate(
                    [jnp.where(first, other_ref[z, at, :], own_ref[z, at, :]) for z in range(8)],
                    axis=0,
                )
            )
        weight = jnp.concatenate(tiles, axis=1)
        kv = jnp.dot(enc, weight, preferred_element_type=F32).astype(BF)
        kv_ref[2 * couple] = kv[:, :128]
        kv_ref[2 * couple + 1] = kv[:, 128:]
    lane = lax.broadcasted_iota(jnp.int32, (1, 768), 1)
    key_view = lane // 192
    key_row = first_row - 1 + (lane % 192) // 32
    for r in range(4):
        low = jnp.zeros((1, 768), jnp.int32)
        high = jnp.zeros((1, 768), jnp.int32)
        for u in range(4):
            mine = key_view == u
            low = jnp.where(mine, start_ref[r, u], low)
            high = jnp.where(mine, jnp.where(seen_ref[u] == 1, end_ref[r, u], -1), high)
        bias = jnp.where((low <= key_row) & (key_row < high), 0.0, -1e30)
        bias_ref[r * 32 : (r + 1) * 32, :] = jnp.broadcast_to(bias, (32, 768))
    left = lax.broadcasted_iota(jnp.int32, (128, 128), 1) < HEAD_DIM
    square = jnp.zeros((128, 1), F32)
    copies = []
    for pair in range(6):
        q = q_ref[:, pair * 128 : (pair + 1) * 128]
        zero = jnp.zeros_like(q)
        keys = kv_ref[pair]
        values = kv_ref[6 + pair]
        both = jnp.concatenate([jnp.where(left, q, zero), jnp.where(left, zero, q)], axis=0)
        scores = lax.dot_general(
            both, keys, (((1,), (1,)), ((), ())), preferred_element_type=F32
        )
        bias = bias_ref[...]
        scores = scores * HEAD_DIM ** (-0.5) + jnp.concatenate([bias, bias], axis=0)
        weights = jnp.exp(scores - jnp.max(scores, axis=-1, keepdims=True))
        share = 1.0 / jnp.sum(weights, axis=-1, keepdims=True)
        outs = jnp.dot(weights.astype(BF), values, preferred_element_type=F32) * share
        attended = jnp.where(left, outs[:128], outs[128:])
        cols = slice(pair * 128, (pair + 1) * 128)
        residual = stream_ref[:, cols].astype(F32) + attended
        residual_ref[:, cols] = residual
        copies.append(
            pltpu.make_async_copy(residual_ref.at[:, cols], far_ref.at[:, cols], sems.at[pair])
        )
        copies[-1].start()
        square = square + jnp.sum(residual * residual, axis=-1, keepdims=True)
    scale = lax.rsqrt(square * (1.0 / 768) + 1e-6)
    normed_ref[...] = (residual_ref[...] * scale * gain_ref[...]).astype(BF)
    for copy in copies:
        copy.wait()


def gelu(v):
    return 0.5 * v * (1.0 + jnp.tanh(0.7978845608028654 * (v + 0.044715 * (v * v * v))))


def two_blocks(where_ref, tok_ref, w_ref, out_refs, chip_flip):
    blocks = []
    for flip in range(2):
        view = where_ref[2] ^ (chip_flip * 2 + flip)
        blocks.append(tok_ref[pl.ds(pl.multiple_of(view * 128, 128), 128), :])

    def gathered(at):
        tiles = []
        for tile in range(6):
            rows = slice(at + tile * 96, at + (tile + 1) * 96)
            tiles.append(jnp.concatenate([w_ref[d, rows, :] for d in range(8)], axis=0))
        return jnp.concatenate(tiles, axis=1)

    tokens = jnp.concatenate(blocks, axis=0)
    hidden = gelu(jnp.dot(tokens, gathered(0), preferred_element_type=F32)).astype(BF)
    parts = last_dims(hidden, gathered(576)).astype(BF)
    for k, out_ref in enumerate(out_refs):
        out_ref[...] = parts[k * 128 : (k + 1) * 128]


def far_kernel(where_ref, tok_ref, w_ref, same_ref, cross_ref):
    two_blocks(where_ref, tok_ref, w_ref, (same_ref, cross_ref), 1)


def near_kernel(where_ref, tok_ref, w_ref, own_ref, sibling_ref, swap_ref):
    two_blocks(where_ref, tok_ref, w_ref, (own_ref, sibling_ref), 0)
    swap_ref[...] = one_hot(768, 6)


def swap_kernel(where_ref, tok_ref, out_ref):
    @pl.when(where_ref[0] == 0)
    def _():
        out_ref[...] = tok_ref[...]

    @pl.when(where_ref[0] != 0)
    def _():
        out_ref[...] = jnp.dot(tok_ref[...], one_hot(768, 6), preferred_element_type=F32).astype(BF)


def sum_kernel(
    where_ref, own_ref, sibling_ref, same_ref, cross_ref, swap_ref, residual_ref, out_ref
):
    alike = own_ref[...].astype(F32) + same_ref[...].astype(F32)
    unlike = sibling_ref[...].astype(F32) + cross_ref[...].astype(F32)
    first = where_ref[0] == 0
    odd = jnp.where(first, unlike, alike)
    even = jnp.where(first, alike, unlike)
    high = odd.astype(BF)
    low = (odd - high.astype(F32)).astype(BF)
    both = last_dims(jnp.concatenate([high, low], axis=0), swap_ref[...])
    odd = both[:128] + both[128:]
    out_ref[...] = (residual_ref[...] + (even + odd)).astype(BF)


def last_dims(a, b):
    return lax.dot_general(a, b, (((1,), (1,)), ((), ())), preferred_element_type=F32)


def pack_kernel(where_ref, *refs):
    (sources, out_ref, held, sems) = (refs[:4], refs[4], refs[5:9], refs[9])
    copies = [pltpu.make_async_copy(sources[k], held[k], sems.at[k]) for k in range(4)]
    for copy in copies:
        copy.start()
    for copy in copies:
        copy.wait()
    conv_ref, kv_ref, up_ref, down_ref = held

    def tiles(ref, count):
        return [ref[:, t * 128 : (t + 1) * 128].astype(F32) for t in range(count)]

    mlp = tiles(up_ref, 6) + tiles(down_ref, 6)

    def put(code):
        block = jnp.concatenate(code + mlp, axis=0).astype(BF)
        for k in range(16):
            out_ref[k] = block

    @pl.when(where_ref[0] == 0)
    def _():
        low, high = tiles(conv_ref, 2)
        half = jnp.where((where_ref[2] >> 1) == 0, low, high)
        put([half, jnp.zeros((6, 128), F32)])

    @pl.when(where_ref[0] != 0)
    def _():
        put(tiles(kv_ref, 12))


def kernel_call(body, out_shape, in_specs, scratch=(), out_specs=None):
    outs = out_specs or jax.tree.map(lambda _: VMEM, out_shape)
    return pl.pallas_call(
        body,
        out_shape=out_shape,
        in_specs=in_specs,
        out_specs=outs,
        scratch_shapes=scratch,
        compiler_params=pltpu.CompilerParams(vmem_limit_bytes=16 << 20),
    )


def in_hbm(value):
    return pltpu.with_memory_space_constraint(value, pltpu.HBM)


def by_core(even, odd):
    ids = np.arange(512).reshape(8, 2, 8, 4)
    groups = []
    for axes, views in ((even, (0, 2)), (odd, (1, 3))):
        held = [axis for axis in range(3) if axis not in axes]
        for view in views:
            lines = ids[..., view].transpose(*held, *axes)
            groups.extend(lines.reshape(-1, int(np.prod([ids.shape[a] for a in axes]))).tolist())
    return groups


def to_view(value, flip):
    return lax.ppermute(value, "view", [(i, i ^ flip) for i in range(4)])


def copies_of(value, count):
    return jnp.broadcast_to(value, (count, *value.shape))


def exchange(copies, groups):
    return lax.all_to_all(
        copies,
        ("dp", "slab_0", "slab_1", "view"),
        split_axis=0,
        concat_axis=0,
        axis_index_groups=groups,
        tiled=True,
    )


def regroup(tiles, rows):
    devices = tiles.shape[0]
    tiles = tiles.reshape(devices, -1, rows, 128).swapaxes(0, 1)
    return tiles.reshape(-1, 128)


def shards(
    latent_feats,
    conv_weight,
    kv_weight,
    stream,
    queries,
    norm_gain,
    up_weight,
    down_weight,
    band_start,
    band_end,
    visibility,
):
    view_id = lax.axis_index("view")
    core = view_id % 2
    first_row = lax.axis_index(SLAB) * 4
    where = jnp.stack([core, first_row, view_id]).astype(jnp.int32)
    feats = latent_feats[0, 0]
    ends = lax.axis_size(SLAB) - 1
    above = lax.ppermute(feats[2:], SLAB, [(i, i + 1) for i in range(ends)])
    below = lax.ppermute(feats[:2], SLAB, [(i + 1, i) for i in range(ends)])
    rows = jnp.concatenate([above, feats, below], axis=0).reshape(256, 256)
    even = core == 0
    mine = kernel_call(
        pack_kernel,
        jax.ShapeDtypeStruct((16, 96, 128), BF),
        [SMEM] + [HBM] * 4,
        scratch=[pltpu.VMEM(w.shape, BF) for w in (conv_weight, kv_weight, up_weight, down_weight)]
        + [pltpu.SemaphoreType.DMA((4,))],
    )(where, *map(in_hbm, (conv_weight, kv_weight, up_weight, down_weight)))
    wide = by_core((1, 2), (0, 1))
    long = by_core((0,), (2,))
    near = exchange(mine, wide)
    code = jnp.where(
        even, jnp.pad(regroup(near[:, :18], 18), ((0, 96), (0, 0))), regroup(near[:, :24], 2)
    )
    units = jnp.concatenate([regroup(near[:, 24:60], 6), regroup(near[:, 60:], 6)], axis=0)
    code = copies_of(code, 8)
    own = exchange(code, long)
    rows = jnp.concatenate([rows, to_view(rows, 2)], axis=0)
    units = copies_of(units, 8)
    other = to_view(own, 1)
    mlp = exchange(units, long)

    encoded = kernel_call(
        conv_kernel,
        jax.ShapeDtypeStruct((384, 128), BF),
        [SMEM, HBM, VMEM, VMEM],
        scratch=[
            pltpu.VMEM((512, 256), BF),
            pltpu.SemaphoreType.DMA(()),
        ],
    )(where, in_hbm(rows), own, other)
    nearby = lax.all_gather(encoded, "view", axis=0, tiled=True)
    vis_row = lax.dynamic_index_in_dim(visibility[0], view_id, 0, False)
    seen = jnp.where(jnp.arange(4) == view_id, 1, vis_row).astype(jnp.int32)
    normed, residual = kernel_call(
        attention_kernel,
        (jax.ShapeDtypeStruct((128, 768), BF), pltpu.HBM((128, 768), F32)),
        [SMEM, SMEM, SMEM, SMEM] + [VMEM] * 6,
        scratch=[
            pltpu.VMEM((12, 768, 128), BF),
            pltpu.VMEM((128, 768), F32),
            pltpu.VMEM((128, 768), F32),
            pltpu.SemaphoreType.DMA((6,)),
        ],
        out_specs=(VMEM, HBM),
    )(
        where,
        band_start[0, 0],
        band_end[0, 0],
        seen,
        nearby,
        own,
        other,
        queries[0, 0].reshape(128, 768),
        stream[0, 0].reshape(128, 768),
        norm_gain.reshape(1, 768),
    )
    tokens = lax.all_gather(normed, "view", axis=0, tiled=True)
    tokens = kernel_call(
        swap_kernel, jax.ShapeDtypeStruct((512, 768), BF), [SMEM, VMEM]
    )(where, tokens)
    block = jax.ShapeDtypeStruct((128, 768), BF)
    square = jax.ShapeDtypeStruct((768, 768), BF)
    same, cross = kernel_call(far_kernel, (block, block), [SMEM, VMEM, VMEM])(where, tokens, mlp)
    cross = to_view(cross, 3)
    same = to_view(same, 2)
    own, sibling, swap = kernel_call(
        near_kernel, (block, block, square), [SMEM, VMEM, VMEM]
    )(where, tokens, mlp)
    sibling = to_view(sibling, 1)
    result = kernel_call(
        sum_kernel, block, [SMEM] + [VMEM] * 6
    )(where, own, sibling, same, cross, swap, residual)
    return result.reshape(1, 1, 4, 32, 768)


def solution(mesh):
    finer = Mesh(
        mesh.devices.reshape(mesh.shape["dp"], 2, 8, mesh.shape["view"]),
        ("dp", "slab_0", "slab_1", "view"),
    )
    in_specs = (
        P("dp", "view", SLAB, None, None),
        P(DP_SLAB, None),
        P(DP_SLAB, None),
        P("dp", "view", SLAB, None, None),
        P("dp", "view", SLAB, None, None),
        P(),
        P(DP_SLAB, "view"),
        P(DP_SLAB, "view"),
        P("dp", "view", SLAB, None),
        P("dp", "view", SLAB, None),
        P("dp", None, None),
    )
    out_specs = P("dp", "view", SLAB, None, None)
    return jax.shard_map(
        shards, mesh=finer, in_specs=in_specs, out_specs=out_specs, check_vma=False
    )
```
